32 devices in a mesh: dp: 1 (over z), tp: 4 (over y), ep: 8 (over x, core).
Axes of the slice: x: 4, y: 4, z: 1, core: 2. Of those that a mesh axis runs over, the one named last changes fastest.
The devices are a block of a 4x4x8 slice.
Arguments:
- emb: bfloat16 [2, 256, 2048], P(None, ('dp', 'ep'))
- pos: int32 [256], P(('dp', 'ep'))
- route_ids: int32 [2, 256, 6], P(None, ('dp', 'ep'))
- lat_cache: bfloat16 [2, 256, 128, 512], P(None, ('dp', 'ep'))
- rope_cache: bfloat16 [2, 256, 128, 64], P(None, ('dp', 'ep'))
- attn_norm: float32 [2, 2048], replicated
- w_q: bfloat16 [2, 2048, 16, 192], P(None, None, 'tp')
- w_dkv: bfloat16 [2, 2048, 576], replicated
- kv_norm: float32 [2, 512], replicated
- w_uk: bfloat16 [2, 512, 16, 128], P(None, None, 'tp')
- w_uv: bfloat16 [2, 512, 16, 128], P(None, None, 'tp')
- w_o: bfloat16 [2, 2048, 2048], P(None, 'tp')
- mlp_norm: float32 [2, 2048], replicated
- dense_gate: bfloat16 [2048, 11264], P(None, 'tp')
- dense_up: bfloat16 [2048, 11264], P(None, 'tp')
- dense_down: bfloat16 [11264, 2048], P('tp')
- router: bfloat16 [2048, 64], replicated
- shared_gate: bfloat16 [2048, 2816], P(None, 'tp')
- shared_up: bfloat16 [2048, 2816], P(None, 'tp')
- shared_down: bfloat16 [2816, 2048], P('tp')
- expert_gate: bfloat16 [64, 2048, 1408], P('ep', None, 'tp')
- expert_up: bfloat16 [64, 2048, 1408], P('ep', None, 'tp')
- expert_down: bfloat16 [64, 1408, 2048], P('ep', 'tp')
Outputs:
- output 1: bfloat16 [2, 256, 2048], P(None, ('dp', 'ep'))
- output 2: bfloat16 [2, 256, 128, 512], P(None, ('dp', 'ep'))
- output 3: bfloat16 [2, 256, 128, 64], P(None, ('dp', 'ep'))
All inputs are finite; a program needn't handle non-finite values.
Results may differ from the reference program's by a relative error of at most 0.02.
Values are sent between devices in bfloat16 or wider.
A program may use at most 768 MiB of HBM per device.

```python
import math
import jax
import jax.numpy as jnp
from jax import lax

HIDDEN = 2048
NUM_HEADS = 16
NOPE_DIM = 128
ROPE_DIM = 64
KV_LORA = 512
V_HEAD = 128
DENSE_FF = 11264
EXPERTS = 64
EXPERT_FF = 1408
SHARED_FF = 2816
TOP_K = 6
TOKENS = 256
CACHE_LEN = 128

QK_DIM = NOPE_DIM + ROPE_DIM
SCORE_SCALE = 1.0 / math.sqrt(QK_DIM)
NORM_EPS = 1e-6
ROPE_THETA = 10000.0
ROUTE_SCALE = 1.5 * EXPERTS / TOP_K
LATENT_GAIN = 0.5 * math.log(CACHE_LEN)


def rms_norm(values, gain):
    wide = values.astype(jnp.float32)
    mean_sq = jnp.mean(wide * wide, axis=-1, keepdims=True)
    return (wide * lax.rsqrt(mean_sq + NORM_EPS) * gain).astype(jnp.bfloat16)


def rope_tables(position):
    half_dim = ROPE_DIM // 2
    inv_freq = ROPE_THETA ** (-(jnp.arange(half_dim, dtype=jnp.float32) * 2.0 / ROPE_DIM))
    angles = position.astype(jnp.float32)[:, None] * inv_freq[None, :]
    return jnp.cos(angles), jnp.sin(angles)


def rotary(values, cos_t, sin_t):
    wide = values.astype(jnp.float32)
    half_dim = wide.shape[-1] // 2
    first = wide[..., :half_dim]
    second = wide[..., half_dim:]
    return jnp.concatenate([first * cos_t - second * sin_t, second * cos_t + first * sin_t], axis=-1)


def attention(hidden, cur_pos, lat, rop, g_attn, w_query, w_dkv, g_kv, w_uk, w_uv, w_out):
    tokens = hidden.shape[0]
    cos_t, sin_t = rope_tables(cur_pos)
    normed = rms_norm(hidden, g_attn)
    query = jnp.dot(normed, w_query.reshape(HIDDEN, NUM_HEADS * QK_DIM), preferred_element_type=jnp.float32).reshape(tokens, NUM_HEADS, QK_DIM)
    q_nope = query[..., :NOPE_DIM].astype(jnp.bfloat16)
    q_rope = rotary(query[..., NOPE_DIM:], cos_t[:, None, :], sin_t[:, None, :]).astype(jnp.bfloat16)
    kv_proj = jnp.dot(normed, w_dkv, preferred_element_type=jnp.float32)
    lat_new = rms_norm(kv_proj[:, :KV_LORA], g_kv)
    rope_new = rotary(kv_proj[:, KV_LORA:], cos_t, sin_t).astype(jnp.bfloat16)
    slot_ids = jnp.arange(CACHE_LEN)
    hit_mask = (slot_ids[None, :] == cur_pos[:, None])[:, :, None]
    lat = jnp.where(hit_mask, lat_new[:, None, :], lat)
    rop = jnp.where(hit_mask, rope_new[:, None, :], rop)
    q_lat = jnp.einsum('bhn,chn->bhc', q_nope.astype(jnp.float32), w_uk.astype(jnp.float32)).astype(jnp.bfloat16)
    lat_wide = lat.astype(jnp.float32)
    scores = (jnp.einsum('bhc,btc->bht', q_lat.astype(jnp.float32), lat_wide) + jnp.einsum('bhr,btr->bht', q_rope.astype(jnp.float32), rop.astype(jnp.float32))) * SCORE_SCALE
    visible = slot_ids[None, None, :] <= cur_pos[:, None, None]
    scores = jnp.where(visible, scores, -1e30)
    prob_bf = jax.nn.softmax(scores, axis=-1).astype(jnp.bfloat16)
    o_lat = jnp.einsum('bht,btc->bhc', prob_bf.astype(jnp.float32), lat_wide).astype(jnp.bfloat16)
    heads_out = jnp.einsum('bhc,chv->bhv', o_lat.astype(jnp.float32), w_uv.astype(jnp.float32)).astype(jnp.bfloat16)
    attn_sum = jnp.dot(heads_out.reshape(tokens, NUM_HEADS * V_HEAD), w_out, preferred_element_type=jnp.float32)
    return (hidden.astype(jnp.float32) + attn_sum).astype(jnp.bfloat16), lat, rop


def swiglu(normed, w_gate, w_up, w_down):
    gate_h = jnp.dot(normed, w_gate, preferred_element_type=jnp.float32)
    up_h = jnp.dot(normed, w_up, preferred_element_type=jnp.float32)
    act_bf = (jax.nn.silu(gate_h) * up_h).astype(jnp.bfloat16)
    return jnp.dot(act_bf, w_down, preferred_element_type=jnp.float32)


def routed(normed, expert_ids, router, expert_gate, expert_up, expert_down):
    logits = jnp.dot(normed, router, preferred_element_type=jnp.float32)
    probs_all = jax.nn.softmax(logits, axis=-1)
    route_w = jnp.take_along_axis(probs_all, expert_ids, axis=1)
    combine = jnp.sum(route_w[:, :, None] * (expert_ids[:, :, None] == jnp.arange(EXPERTS)[None, None, :]), axis=1)

    def expert_step(total, packed):
        gate_w, up_w, down_w, weight_col = packed
        return total + weight_col[:, None] * swiglu(normed, gate_w, up_w, down_w), None

    start_sum = jnp.zeros((normed.shape[0], HIDDEN), jnp.float32)
    return lax.scan(expert_step, start_sum, (expert_gate, expert_up, expert_down, combine.T))[0]


def setup_inputs(seed: int = 0, part: int = 0) -> dict:
    base = jax.random.key(seed)
    part_keys = jax.random.split(jax.random.fold_in(base, part), 8)
    weight_keys = jax.random.split(jax.random.fold_in(base, 100003), 18)

    def normal(key, shape):
        return jax.random.normal(key, shape, jnp.float32)

    emb = normal(part_keys[0], (2, TOKENS, HIDDEN)).astype(jnp.bfloat16)
    pos = jax.random.randint(part_keys[1], (TOKENS,), 1, CACHE_LEN - 1, dtype=jnp.int32).at[0].set(CACHE_LEN - 2)
    hot_bias = jax.random.randint(part_keys[2], (EXPERTS,), 0, 3, dtype=jnp.int32) * 64
    raw_score = jax.random.randint(part_keys[3], (2, TOKENS, EXPERTS), 0, 128, dtype=jnp.int32) + hot_bias
    keyed = raw_score * EXPERTS + jnp.arange(EXPERTS, dtype=jnp.int32)
    route_ids = lax.top_k(keyed, TOP_K)[1].astype(jnp.int32)
    lat_cache = (0.5 * normal(part_keys[4], (2, TOKENS, 1, KV_LORA)) + 0.2 * normal(part_keys[5], (2, TOKENS, CACHE_LEN, KV_LORA))).astype(jnp.bfloat16)
    rope_cache = (1.5 * normal(part_keys[6], (2, TOKENS, 1, ROPE_DIM)) + 0.3 * normal(part_keys[7], (2, TOKENS, CACHE_LEN, ROPE_DIM))).astype(jnp.bfloat16)
    q_scale = jnp.where(jnp.arange(QK_DIM) < NOPE_DIM, 1.0, 2.0) * HIDDEN ** -0.5
    return dict(
        emb=emb,
        pos=pos,
        route_ids=route_ids,
        lat_cache=lat_cache,
        rope_cache=rope_cache,
        attn_norm=1.0 + 0.25 * normal(weight_keys[0], (2, HIDDEN)),
        w_q=(normal(weight_keys[1], (2, HIDDEN, NUM_HEADS, QK_DIM)) * q_scale).astype(jnp.bfloat16),
        w_dkv=(normal(weight_keys[2], (2, HIDDEN, KV_LORA + ROPE_DIM)) * HIDDEN ** -0.5).astype(jnp.bfloat16),
        kv_norm=1.0 + 0.25 * normal(weight_keys[3], (2, KV_LORA)),
        w_uk=(normal(weight_keys[4], (2, KV_LORA, NUM_HEADS, NOPE_DIM)) * (LATENT_GAIN * NOPE_DIM ** -0.5)).astype(jnp.bfloat16),
        w_uv=(normal(weight_keys[5], (2, KV_LORA, NUM_HEADS, V_HEAD)) * KV_LORA ** -0.5).astype(jnp.bfloat16),
        w_o=(normal(weight_keys[6], (2, NUM_HEADS * V_HEAD, HIDDEN)) * (NUM_HEADS * V_HEAD) ** -0.5).astype(jnp.bfloat16),
        mlp_norm=1.0 + 0.25 * normal(weight_keys[7], (2, HIDDEN)),
        dense_gate=(normal(weight_keys[8], (HIDDEN, DENSE_FF)) * HIDDEN ** -0.5).astype(jnp.bfloat16),
        dense_up=(normal(weight_keys[9], (HIDDEN, DENSE_FF)) * HIDDEN ** -0.5).astype(jnp.bfloat16),
        dense_down=(normal(weight_keys[10], (DENSE_FF, HIDDEN)) * DENSE_FF ** -0.5).astype(jnp.bfloat16),
        router=(normal(weight_keys[11], (HIDDEN, EXPERTS)) * (1.5 * HIDDEN ** -0.5)).astype(jnp.bfloat16),
        shared_gate=(normal(weight_keys[12], (HIDDEN, SHARED_FF)) * HIDDEN ** -0.5).astype(jnp.bfloat16),
        shared_up=(normal(weight_keys[13], (HIDDEN, SHARED_FF)) * HIDDEN ** -0.5).astype(jnp.bfloat16),
        shared_down=(normal(weight_keys[14], (SHARED_FF, HIDDEN)) * SHARED_FF ** -0.5).astype(jnp.bfloat16),
        expert_gate=(normal(weight_keys[15], (EXPERTS, HIDDEN, EXPERT_FF)) * HIDDEN ** -0.5).astype(jnp.bfloat16),
        expert_up=(normal(weight_keys[16], (EXPERTS, HIDDEN, EXPERT_FF)) * HIDDEN ** -0.5).astype(jnp.bfloat16),
        expert_down=(normal(weight_keys[17], (EXPERTS, EXPERT_FF, HIDDEN)) * (ROUTE_SCALE * EXPERT_FF ** -0.5)).astype(jnp.bfloat16),
    )


def reference(emb, pos, route_ids, lat_cache, rope_cache, attn_norm, w_q, w_dkv, kv_norm, w_uk, w_uv, w_o, mlp_norm, dense_gate, dense_up, dense_down, router, shared_gate, shared_up, shared_down, expert_gate, expert_up, expert_down):
    lat_first, lat_second = lat_cache[0], lat_cache[1]
    rop_first, rop_second = rope_cache[0], rope_cache[1]
    hidden_steps = []
    for step_idx in range(2):
        cur_pos = pos + step_idx
        y_first, lat_first, rop_first = attention(emb[step_idx], cur_pos, lat_first, rop_first, attn_norm[0], w_q[0], w_dkv[0], kv_norm[0], w_uk[0], w_uv[0], w_o[0])
        dense_out = swiglu(rms_norm(y_first, mlp_norm[0]), dense_gate, dense_up, dense_down)
        h_mid = (y_first.astype(jnp.float32) + dense_out).astype(jnp.bfloat16)
        y_second, lat_second, rop_second = attention(h_mid, cur_pos, lat_second, rop_second, attn_norm[1], w_q[1], w_dkv[1], kv_norm[1], w_uk[1], w_uv[1], w_o[1])
        normed = rms_norm(y_second, mlp_norm[1])
        moe_out = swiglu(normed, shared_gate, shared_up, shared_down) + routed(normed, route_ids[step_idx], router, expert_gate, expert_up, expert_down)
        hidden_steps.append((y_second.astype(jnp.float32) + moe_out).astype(jnp.bfloat16))
    return jnp.stack(hidden_steps), jnp.stack([lat_first, lat_second]), jnp.stack([rop_first, rop_second])
```

```python
import functools
import math

import jax
import jax.numpy as jnp
from jax import lax
from jax.experimental import pallas as pl
from jax.experimental.pallas import tpu as pltpu
from jax.sharding import PartitionSpec as P

NORM_EPS = 1e-6
ROPE_THETA = 10000.0
F32 = jnp.float32
BF16 = jnp.bfloat16
MESH = pl.DeviceIdType.MESH
VMEM = pl.BlockSpec(memory_space=pltpu.VMEM)
NT = (((1,), (1,)), ((), ()))
PAIR = 2


def rms_norm(values, gain):
    wide = values.astype(F32)
    mean_sq = jnp.mean(wide * wide, axis=-1, keepdims=True)
    return (wide * lax.rsqrt(mean_sq + NORM_EPS) * gain).astype(BF16)


def silu(x):
    return x * jax.nn.sigmoid(x)


def dot(a, b):
    return jnp.dot(a, b, preferred_element_type=F32)


def dot_nt(a, b):
    return lax.dot_general(a, b, NT, preferred_element_type=F32)


def sum_tp(me, n, rows, part_ref, recv, send_sem, recv_sem):
    copies = []
    for d in [2, 1, 3] if n == 4 else range(1, n):
        peer = lax.rem(me + d, n)
        copies.append(pltpu.make_async_remote_copy(
            src_ref=part_ref.at[pl.ds(peer * rows, rows)], dst_ref=recv.at[d - 1],
            send_sem=send_sem.at[d - 1], recv_sem=recv_sem.at[d - 1],
            device_id={"tp": peer}, device_id_type=MESH))
    for c in copies:
        c.start()
    total = part_ref[pl.ds(me * rows, rows), :]
    for c in copies:
        c.wait_recv()
    for d in range(1, n):
        total = total + recv[d - 1]
    return total, copies


def all_reduce_kernel(n, part_ref, res_ref, y_ref, recv, chunks, s1, r1, s2, r2):
    me = lax.axis_index("tp")
    rows = part_ref.shape[0] // n
    barrier = pltpu.get_barrier_semaphore()
    for d in range(1, n):
        pl.semaphore_signal(barrier, inc=1, device_id={"tp": lax.rem(me + d, n)}, device_id_type=MESH)
    pl.semaphore_wait(barrier, n - 1)
    total, copies = sum_tp(me, n, rows, part_ref, recv, s1, r1)
    mine = (res_ref[pl.ds(me * rows, rows), :].astype(F32) + total).astype(BF16)
    chunks[me] = mine
    outs = []
    for d in range(1, n):
        outs.append(pltpu.make_async_remote_copy(
            src_ref=chunks.at[me], dst_ref=chunks.at[me], send_sem=s2.at[d - 1], recv_sem=r2.at[d - 1],
            device_id={"tp": lax.rem(me + d, n)}, device_id_type=MESH))
    for c in outs:
        c.start()
    for c in copies:
        c.wait_send()
    for d in range(1, n):
        src = lax.rem(me - d + n, n)
        pltpu.make_async_remote_copy(
            src_ref=chunks.at[src], dst_ref=chunks.at[src], send_sem=s2.at[d - 1], recv_sem=r2.at[d - 1],
            device_id={"tp": src}, device_id_type=MESH).wait_recv()
    for c in outs:
        c.wait_send()
    for i in range(n):
        y_ref[pl.ds(i * rows, rows), :] = chunks[i]


def all_reduce(n, cid, part, res):
    tokens, width = part.shape
    rows = tokens // n
    return pl.pallas_call(
        functools.partial(all_reduce_kernel, n),
        out_shape=jax.ShapeDtypeStruct((tokens, width), BF16),
        in_specs=[VMEM] * 2, out_specs=VMEM,
        scratch_shapes=[pltpu.VMEM((n - 1, rows, width), F32), pltpu.VMEM((n, rows, width), BF16)]
        + [pltpu.SemaphoreType.DMA((n - 1,))] * 4,
        compiler_params=pltpu.CompilerParams(collective_id=cid, has_side_effects=True),
        name="all_reduce_tp",
    )(part, res)


def dispatch_kernel(nt, nx, part_ref, res_ref, gain_ref, mask_ref, y_ref, tok_ref, recv, s1, r1, sx, rx, sy, ry, sd, rd):
    t = lax.axis_index("tp")
    ep = lax.axis_index("ep")
    x, c = ep // PAIR, lax.rem(ep, PAIR)
    sib = {"ep": x * PAIR + 1 - c}
    rows = y_ref.shape[0]
    width = part_ref.shape[1]
    half = width // 2
    total_w = tok_ref.shape[-1]
    lo, hi = pl.ds(0, half), pl.ds(half, total_w - half)
    tp_peer = [lax.rem(t + d, nt) for d in range(1, nt)]
    tp_src = [lax.rem(t - d + nt, nt) for d in range(1, nt)]
    x_peer = [lax.rem(x + d, nx) for d in range(1, nx)]
    x_src = [lax.rem(x - d + nx, nx) for d in range(1, nx)]

    barrier = pltpu.get_barrier_semaphore()
    for p in tp_peer:
        pl.semaphore_signal(barrier, inc=1, device_id={"tp": p}, device_id_type=MESH)
    for p in x_peer:
        pl.semaphore_signal(barrier, inc=1, device_id={"ep": p * PAIR + c}, device_id_type=MESH)
    pl.semaphore_signal(barrier, inc=1, device_id=sib, device_id_type=MESH)
    pl.semaphore_wait(barrier, nt + nx - 1)

    total, first = sum_tp(t, nt, rows, part_ref, recv, s1, r1)
    y = (res_ref[pl.ds(t * rows, rows), :].astype(F32) + total).astype(BF16)
    y_ref[...] = y
    tok_ref[x, c, t, :, pl.ds(0, width)] = rms_norm(y, gain_ref[...])
    tok_ref[x, c, t, :, pl.ds(width, total_w - width)] = mask_ref[pl.ds(t * rows, rows), :]

    def rc(ref, ssem, rsem, dev):
        return pltpu.make_async_remote_copy(src_ref=ref, dst_ref=ref, send_sem=ssem, recv_sem=rsem,
                                            device_id=dev, device_id_type=MESH)

    def to_x(p):
        return {"ep": p * PAIR + c}

    sends = list(first)
    for d in range(1, nx):
        s = rc(tok_ref.at[x, c, t, :, lo], sx.at[0, d - 1], rx.at[0, d - 1], to_x(x_peer[d - 1]))
        s.start()
        sends.append(s)
    for d in range(1, nt):
        s = rc(tok_ref.at[x, c, t, :, hi], sy.at[0, d - 1], ry.at[0, d - 1], {"tp": tp_peer[d - 1]})
        s.start()
        sends.append(s)
    for d in range(1, nx):
        rc(tok_ref.at[x_src[d - 1], c, t, :, lo], sx.at[0, d - 1], rx.at[0, d - 1], to_x(x_src[d - 1])).wait_recv()
    for d in range(1, nt):
        s = rc(tok_ref.at[:, c, t, :, lo], sy.at[1, d - 1], ry.at[1, d - 1], {"tp": tp_peer[d - 1]})
        s.start()
        sends.append(s)
    s = rc(tok_ref.at[:, c, t, :, lo], sd.at[0], rd.at[0], sib)
    s.start()
    sends.append(s)
    for d in range(1, nt):
        rc(tok_ref.at[x, c, tp_src[d - 1], :, hi], sy.at[0, d - 1], ry.at[0, d - 1], {"tp": tp_src[d - 1]}).wait_recv()
    for d in range(1, nx):
        s = rc(tok_ref.at[x, c, :, :, hi], sx.at[1, d - 1], rx.at[1, d - 1], to_x(x_peer[d - 1]))
        s.start()
        sends.append(s)
    s = rc(tok_ref.at[x, c, :, :, hi], sd.at[1], rd.at[1], sib)
    s.start()
    sends.append(s)
    k = 2
    for d in range(1, nt):
        src = tp_src[d - 1]
        rc(tok_ref.at[:, c, src, :, lo], sy.at[1, d - 1], ry.at[1, d - 1], {"tp": src}).wait_recv()
        s = rc(tok_ref.at[:, c, src, :, lo], sd.at[k], rd.at[k], sib)
        s.start()
        sends.append(s)
        k += 1
    for d in range(1, nx):
        src = x_src[d - 1]
        rc(tok_ref.at[src, c, :, :, hi], sx.at[1, d - 1], rx.at[1, d - 1], to_x(src)).wait_recv()
        s = rc(tok_ref.at[src, c, :, :, hi], sd.at[k], rd.at[k], sib)
        s.start()
        sends.append(s)
        k += 1
    o = 1 - c
    rc(tok_ref.at[:, o, t, :, lo], sd.at[0], rd.at[0], sib).wait_recv()
    rc(tok_ref.at[x, o, :, :, hi], sd.at[1], rd.at[1], sib).wait_recv()
    k = 2
    for d in range(1, nt):
        rc(tok_ref.at[:, o, tp_src[d - 1], :, lo], sd.at[k], rd.at[k], sib).wait_recv()
        k += 1
    for d in range(1, nx):
        rc(tok_ref.at[x_src[d - 1], o, :, :, hi], sd.at[k], rd.at[k], sib).wait_recv()
        k += 1
    for s in sends:
        s.wait_send()


def dispatch(nt, nx, cid, part, res, gain, mask):
    tokens, width = part.shape
    rows = tokens // nt
    total_w = width + mask.shape[1]
    ndd = nt + nx
    return pl.pallas_call(
        functools.partial(dispatch_kernel, nt, nx),
        out_shape=[jax.ShapeDtypeStruct((rows, width), BF16),
                   jax.ShapeDtypeStruct((nx, PAIR, nt, rows, total_w), BF16)],
        in_specs=[VMEM] * 4, out_specs=[VMEM] * 2,
        scratch_shapes=[pltpu.VMEM((nt - 1, rows, width), F32),
                        pltpu.SemaphoreType.DMA((nt - 1,)), pltpu.SemaphoreType.DMA((nt - 1,)),
                        pltpu.SemaphoreType.DMA((2, nx - 1)), pltpu.SemaphoreType.DMA((2, nx - 1)),
                        pltpu.SemaphoreType.DMA((2, nt - 1)), pltpu.SemaphoreType.DMA((2, nt - 1)),
                        pltpu.SemaphoreType.DMA((ndd,)), pltpu.SemaphoreType.DMA((ndd,))],
        compiler_params=pltpu.CompilerParams(collective_id=cid, has_side_effects=True),
        name="dispatch_tokens",
    )(part, res, gain.reshape(1, -1), mask)


def combine_kernel(nt, nx, part_ref, y_ref, out_ref, half_in, sums, ax, ay, bx, by, own, chunks,
                   sd, rd, sx, rx, sy, ry, so, ro):
    t = lax.axis_index("tp")
    ep = lax.axis_index("ep")
    x, c = ep // PAIR, lax.rem(ep, PAIR)
    o = 1 - c
    sib = {"ep": x * PAIR + o}
    rows, width = y_ref.shape
    half = width // 2
    lo, hi = pl.ds(0, half), pl.ds(half, half)
    tp_peer = [lax.rem(t + d, nt) for d in range(1, nt)]
    tp_src = [lax.rem(t - d + nt, nt) for d in range(1, nt)]
    x_peer = [lax.rem(x + d, nx) for d in range(1, nx)]

    barrier = pltpu.get_barrier_semaphore()
    for p in tp_peer:
        pl.semaphore_signal(barrier, inc=1, device_id={"tp": p}, device_id_type=MESH)
    for p in x_peer:
        pl.semaphore_signal(barrier, inc=1, device_id={"ep": p * PAIR + c}, device_id_type=MESH)
    pl.semaphore_signal(barrier, inc=1, device_id=sib, device_id_type=MESH)
    pl.semaphore_wait(barrier, nt + nx - 1)

    def rc(src, dst, ssem, rsem, dev):
        return pltpu.make_async_remote_copy(src_ref=src, dst_ref=dst, send_sem=ssem, recv_sem=rsem,
                                            device_id=dev, device_id_type=MESH)

    sends = []
    pair = []
    for i in range(nx):
        s = rc(part_ref.at[i, o], half_in.at[i], sd.at[i], rd.at[i], sib)
        s.start()
        pair.append(s)
    for i in range(nx):
        pair[i].wait_recv()
        sums[i] = part_ref[i, c] + half_in[i]
    stage1x, stage1y = [], []
    for d in range(1, nx):
        s = rc(sums.at[x_peer[d - 1], :, :, lo], ax.at[d - 1], sx.at[0, d - 1], rx.at[0, d - 1], {"ep": x_peer[d - 1] * PAIR + c})
        s.start()
        stage1x.append(s)
    for d in range(1, nt):
        s = rc(sums.at[:, tp_peer[d - 1], :, hi], ay.at[d - 1], sy.at[0, d - 1], ry.at[0, d - 1], {"tp": tp_peer[d - 1]})
        s.start()
        stage1y.append(s)
    for s in stage1x:
        s.wait_recv()
    low = sums[x, :, :, lo]
    for d in range(1, nx):
        low = low + ax[d - 1]
    bx[...] = low
    stage2 = []
    for d in range(1, nt):
        s = rc(bx.at[tp_peer[d - 1]], own.at[0, d - 1], sy.at[1, d - 1], ry.at[1, d - 1], {"tp": tp_peer[d - 1]})
        s.start()
        stage2.append(s)
    for s in stage1y:
        s.wait_recv()
    high = sums[:, t, :, hi]
    for d in range(1, nt):
        high = high + ay[d - 1]
    by[...] = high
    for d in range(1, nx):
        s = rc(by.at[x_peer[d - 1]], own.at[1, d - 1], sx.at[1, d - 1], rx.at[1, d - 1], {"ep": x_peer[d - 1] * PAIR + c})
        s.start()
        stage2.append(s)
    for s in stage2:
        s.wait_recv()
    low = bx[t] + y_ref[:, :half].astype(F32)
    for d in range(1, nt):
        low = low + own[0, d - 1]
    high = by[x] + y_ref[:, half:].astype(F32)
    for d in range(1, nx):
        high = high + own[1, d - 1]
    chunks[t, :, lo] = low.astype(BF16)
    chunks[t, :, hi] = high.astype(BF16)
    outs = []
    for d in range(1, nt):
        s = rc(chunks.at[t], chunks.at[t], so.at[d - 1], ro.at[d - 1], {"tp": tp_peer[d - 1]})
        s.start()
        outs.append(s)
    for d in range(1, nt):
        rc(chunks.at[tp_src[d - 1]], chunks.at[tp_src[d - 1]], so.at[d - 1], ro.at[d - 1], {"tp": tp_src[d - 1]}).wait_recv()
    for s in pair + stage1x + stage1y + stage2 + outs:
        s.wait_send()
    out_ref[...] = chunks[...]


def combine(nt, nx, cid, part, y):
    rows, width = y.shape
    half = width // 2
    return pl.pallas_call(
        functools.partial(combine_kernel, nt, nx),
        out_shape=jax.ShapeDtypeStruct((nt, rows, width), BF16),
        in_specs=[VMEM] * 2, out_specs=VMEM,
        scratch_shapes=[pltpu.VMEM((nx, nt, rows, width), F32), pltpu.VMEM((nx, nt, rows, width), F32),
                        pltpu.VMEM((nx - 1, nt, rows, half), F32), pltpu.VMEM((nt - 1, nx, rows, half), F32),
                        pltpu.VMEM((nt, rows, half), F32), pltpu.VMEM((nx, rows, half), F32),
                        pltpu.VMEM((2, max(nt, nx) - 1, rows, half), F32),
                        pltpu.VMEM((nt, rows, width), BF16),
                        pltpu.SemaphoreType.DMA((nx,)), pltpu.SemaphoreType.DMA((nx,)),
                        pltpu.SemaphoreType.DMA((2, nx - 1)), pltpu.SemaphoreType.DMA((2, nx - 1)),
                        pltpu.SemaphoreType.DMA((2, nt - 1)), pltpu.SemaphoreType.DMA((2, nt - 1)),
                        pltpu.SemaphoreType.DMA((nt - 1,)), pltpu.SemaphoreType.DMA((nt - 1,))],
        compiler_params=pltpu.CompilerParams(collective_id=cid, has_side_effects=True, vmem_limit_bytes=40 << 20),
        name="combine_experts",
    )(part, y)


def dense_kernel(y_ref, gain_ref, gate_ref, up_ref, down_ref, out_ref, normed):
    i = pl.program_id(0)

    @pl.when(i == 0)
    def _():
        normed[...] = rms_norm(y_ref[...], gain_ref[...])

    a = normed[...]
    act = (silu(dot(a, gate_ref[...])) * dot(a, up_ref[...])).astype(BF16)
    part = dot(act, down_ref[...])

    @pl.when(i == 0)
    def _():
        out_ref[...] = part

    @pl.when(i > 0)
    def _():
        out_ref[...] += part


def dense_mlp(y, gain, gate, up, down):
    tokens, hidden = y.shape
    width = gate.shape[1]
    tile = 256
    while width % tile:
        tile //= 2
    return pl.pallas_call(
        dense_kernel,
        grid=(width // tile,),
        out_shape=jax.ShapeDtypeStruct((tokens, hidden), F32),
        in_specs=[pl.BlockSpec((tokens, hidden), lambda i: (0, 0)), pl.BlockSpec((1, hidden), lambda i: (0, 0)),
                  pl.BlockSpec((hidden, tile), lambda i: (0, i)), pl.BlockSpec((hidden, tile), lambda i: (0, i)),
                  pl.BlockSpec((tile, hidden), lambda i: (i, 0))],
        out_specs=pl.BlockSpec((tokens, hidden), lambda i: (0, 0)),
        scratch_shapes=[pltpu.VMEM((tokens, hidden), BF16)],
        compiler_params=pltpu.CompilerParams(vmem_limit_bytes=40 << 20),
        name="dense_mlp",
    )(y, gain.reshape(1, -1), gate, up, down)


def moe_kernel(n_exp, own, tok_ref, router_ref, gate_ref, up_ref, down_ref, sg_ref, su_ref, sd_ref, out_ref, comb):
    i = pl.program_id(0)
    ep = lax.axis_index("ep")
    hidden = out_ref.shape[1]
    experts = router_ref.shape[0]
    cols = 512

    @pl.when(i == 0)
    def _():
        logits = dot_nt(tok_ref[:, :hidden], router_ref[...])
        mask = tok_ref[:, hidden:hidden + experts].astype(F32)
        e = jnp.exp(logits - jnp.max(logits, axis=-1, keepdims=True))
        comb[...] = e / jnp.sum(e, axis=-1, keepdims=True) * mask

    @pl.when(i < n_exp)
    def _():
        a = tok_ref[:, :hidden]
        act = (silu(dot_nt(a, gate_ref[0])) * dot_nt(a, up_ref[0])).astype(BF16)
        lane = lax.broadcasted_iota(jnp.int32, comb.shape, 1)
        w = jnp.sum(jnp.where(lane == ep * n_exp + i, comb[...], 0.0), axis=1, keepdims=True)
        for j in range(0, hidden, cols):
            part = w * dot(act, down_ref[0, :, j:j + cols])

            @pl.when(i == 0)
            def _():
                out_ref[:, j:j + cols] = part

            @pl.when(i > 0)
            def _():
                out_ref[:, j:j + cols] += part

    @pl.when(i >= n_exp)
    def _():
        r = pl.ds(pl.multiple_of(ep * own, own), own)
        a = tok_ref[r, :hidden]
        act = (silu(dot_nt(a, sg_ref[...])) * dot_nt(a, su_ref[...])).astype(BF16)
        for j in range(0, hidden, cols):
            out_ref[r, j:j + cols] += dot(act, sd_ref[:, j:j + cols])


def moe(own, tok, router_t, gate_t, up_t, down, sg_t, su_t, sd):
    tokens = tok.shape[0]
    n_exp, width, hidden = gate_t.shape
    steps = sg_t.shape[0] // width
    ex = lambda i: (jnp.minimum(i, n_exp - 1), 0, 0)
    sh = lambda i: (jnp.maximum(i - n_exp, 0), 0)
    return pl.pallas_call(
        functools.partial(moe_kernel, n_exp, own),
        grid=(n_exp + steps,),
        out_shape=jax.ShapeDtypeStruct((tokens, hidden), F32),
        in_specs=[pl.BlockSpec(tok.shape, lambda i: (0, 0)), pl.BlockSpec(router_t.shape, lambda i: (0, 0)),
                  pl.BlockSpec((1, width, hidden), ex), pl.BlockSpec((1, width, hidden), ex),
                  pl.BlockSpec((1, width, hidden), ex),
                  pl.BlockSpec((width, hidden), sh), pl.BlockSpec((width, hidden), sh), pl.BlockSpec((width, hidden), sh)],
        out_specs=pl.BlockSpec((tokens, hidden), lambda i: (0, 0)),
        scratch_shapes=[pltpu.VMEM((tokens, router_t.shape[0]), F32)],
        compiler_params=pltpu.CompilerParams(vmem_limit_bytes=56 << 20),
        name="moe_experts",
    )(tok, router_t, gate_t, up_t, down, sg_t, su_t, sd)


def rope_tables(position, rope_dim):
    half_dim = rope_dim // 2
    inv_freq = ROPE_THETA ** (-(jnp.arange(half_dim, dtype=F32) * 2.0 / rope_dim))
    angles = position.astype(F32)[:, None] * inv_freq[None, :]
    return jnp.cos(angles), jnp.sin(angles)


def rotary(values, cos_t, sin_t):
    wide = values.astype(F32)
    half_dim = wide.shape[-1] // 2
    first = wide[..., :half_dim]
    second = wide[..., half_dim:]
    return jnp.concatenate([first * cos_t - second * sin_t, second * cos_t + first * sin_t], axis=-1)


def attention(hidden, pos, cos_t, sin_t, lat, rop, g_attn, w_query, w_dkv, g_kv, w_uk, w_uv, w_out):
    seqs, slots = lat.shape[:2]
    steps = hidden.shape[0] // seqs
    nope_dim = w_uk.shape[2]
    heads, qk_dim = w_query.shape[1:]
    lora = g_kv.shape[0]
    normed = rms_norm(hidden, g_attn)
    query = jnp.einsum('bd,dhk->bhk', normed, w_query, preferred_element_type=F32)
    q_nope = query[..., :nope_dim].astype(BF16)
    q_rope = rotary(query[..., nope_dim:], cos_t[:, None, :], sin_t[:, None, :]).astype(BF16)
    kv_proj = dot(normed, w_dkv)
    lat_new = rms_norm(kv_proj[:, :lora], g_kv)
    rope_new = rotary(kv_proj[:, lora:], cos_t, sin_t).astype(BF16)
    slot_ids = jnp.arange(slots)
    for s in range(steps):
        hit = (slot_ids[None, :] == (pos + s)[:, None])[:, :, None]
        lat = jnp.where(hit, lat_new[s * seqs:(s + 1) * seqs, None, :], lat)
        rop = jnp.where(hit, rope_new[s * seqs:(s + 1) * seqs, None, :], rop)
    q_lat = jnp.einsum('bhn,chn->bhc', q_nope, w_uk, preferred_element_type=F32).astype(BF16)

    def group(q):
        return q.reshape(steps, seqs, heads, -1).transpose(1, 0, 2, 3).reshape(seqs, steps * heads, -1)

    scores = jnp.einsum('bhc,btc->bht', group(q_lat), lat, preferred_element_type=F32)
    scores = scores + jnp.einsum('bhr,btr->bht', group(q_rope), rop, preferred_element_type=F32)
    scores = scores * (1.0 / math.sqrt(qk_dim))
    step_of = jnp.arange(steps * heads) // heads
    visible = slot_ids[None, None, :] <= pos[:, None, None] + step_of[None, :, None]
    scores = jnp.where(visible, scores, -1e30)
    probs = jax.nn.softmax(scores, axis=-1).astype(BF16)
    o_lat = jnp.einsum('bht,btc->bhc', probs, lat, preferred_element_type=F32).astype(BF16)
    o_lat = o_lat.reshape(seqs, steps, heads, -1).transpose(1, 0, 2, 3).reshape(steps * seqs, heads, -1)
    heads_out = jnp.einsum('bhc,chv->bhv', o_lat, w_uv, preferred_element_type=F32).astype(BF16)
    return dot(heads_out.reshape(steps * seqs, -1), w_out), lat, rop


def solution(mesh):
    tok_axes = ('dp', 'ep')
    nt = mesh.shape['tp']
    nx = mesh.shape['ep'] // PAIR

    def device_fn(emb, pos, route_ids, lat_cache, rope_cache, attn_norm, w_q, w_dkv, kv_norm, w_uk, w_uv, w_o, mlp_norm, dense_gate, dense_up, dense_down, router, shared_gate, shared_up, shared_down, expert_gate, expert_up, expert_down):
        steps, seqs, hidden = emb.shape
        own = steps * seqs
        experts = router.shape[1]
        cur = jnp.concatenate([pos + s for s in range(steps)])
        cos_t, sin_t = rope_tables(cur, rope_cache.shape[-1])
        ids = route_ids.reshape(own, -1)
        lanes = -(-experts // 128) * 128
        mask = jnp.any(ids[:, :, None] == jnp.arange(lanes)[None, None, :], axis=1).astype(BF16)

        h = emb.reshape(own, hidden)
        part, lat0, rop0 = attention(h, pos, cos_t, sin_t, lat_cache[0], rope_cache[0], attn_norm[0], w_q[0], w_dkv[0], kv_norm[0], w_uk[0], w_uv[0], w_o[0])
        y = all_reduce(nt, 0, part, h)
        part = dense_mlp(y, mlp_norm[0], dense_gate, dense_up, dense_down)
        h = all_reduce(nt, 1, part, y)
        part, lat1, rop1 = attention(h, pos, cos_t, sin_t, lat_cache[1], rope_cache[1], attn_norm[1], w_q[1], w_dkv[1], kv_norm[1], w_uk[1], w_uv[1], w_o[1])
        y, tok = dispatch(nt, nx, 2, part, h, mlp_norm[1], mask)
        part = moe(own, tok.reshape(-1, tok.shape[-1]), router.T, expert_gate.transpose(0, 2, 1), expert_up.transpose(0, 2, 1), expert_down, shared_gate.T, shared_up.T, shared_down)
        out = combine(nt, nx, 3, part.reshape(nx, PAIR, nt, own // nt, hidden), y)
        return out.reshape(steps, seqs, hidden), jnp.stack([lat0, lat1]), jnp.stack([rop0, rop1])

    in_specs = (P(None, tok_axes, None), P(tok_axes), P(None, tok_axes, None), P(None, tok_axes, None, None), P(None, tok_axes, None, None), P(), P(None, None, 'tp', None), P(), P(), P(None, None, 'tp', None), P(None, None, 'tp', None), P(None, 'tp', None), P(), P(None, 'tp'), P(None, 'tp'), P('tp', None), P(), P(None, 'tp'), P(None, 'tp'), P('tp', None), P('ep', None, 'tp'), P('ep', None, 'tp'), P('ep', 'tp', None))
    out_specs = (P(None, tok_axes, None), P(None, tok_axes, None, None), P(None, tok_axes, None, None))
    return jax.shard_map(device_fn, mesh=mesh, in_specs=in_specs, out_specs=out_specs, check_vma=False)
```

```python
import functools
import math

import jax
import jax.numpy as jnp
from jax import lax
from jax.experimental import pallas as pl
from jax.experimental.pallas import tpu as pltpu
from jax.sharding import PartitionSpec as P

NORM_EPS = 1e-6
ROPE_THETA = 10000.0
F32 = jnp.float32
BF16 = jnp.bfloat16
MESH = pl.DeviceIdType.MESH
VMEM = pl.BlockSpec(memory_space=pltpu.VMEM)
NT = (((1,), (1,)), ((), ()))
PAIR = 2


def rms_norm(values, gain):
    wide = values.astype(F32)
    mean_sq = jnp.mean(wide * wide, axis=-1, keepdims=True)
    return (wide * lax.rsqrt(mean_sq + NORM_EPS) * gain).astype(BF16)


def silu(x):
    return x * jax.nn.sigmoid(x)


def dot(a, b):
    return jnp.dot(a, b, preferred_element_type=F32)


def dot_nt(a, b):
    return lax.dot_general(a, b, NT, preferred_element_type=F32)


def sum_tp(me, n, rows, part_ref, recv, send_sem, recv_sem):
    copies = []
    for d in [2, 1, 3] if n == 4 else range(1, n):
        peer = lax.rem(me + d, n)
        copies.append(pltpu.make_async_remote_copy(
            src_ref=part_ref.at[pl.ds(peer * rows, rows)], dst_ref=recv.at[d - 1],
            send_sem=send_sem.at[d - 1], recv_sem=recv_sem.at[d - 1],
            device_id={"tp": peer}, device_id_type=MESH))
    for c in copies:
        c.start()
    total = part_ref[pl.ds(me * rows, rows), :]
    for c in copies:
        c.wait_recv()
    for d in range(1, n):
        total = total + recv[d - 1]
    return total, copies


def share(n, me, buf, send_sem, recv_sem):
    outs = []
    for d in range(1, n):
        outs.append(pltpu.make_async_remote_copy(
            src_ref=buf.at[me], dst_ref=buf.at[me], send_sem=send_sem.at[d - 1], recv_sem=recv_sem.at[d - 1],
            device_id={"tp": lax.rem(me + d, n)}, device_id_type=MESH))
    for c in outs:
        c.start()
    for d in range(1, n):
        src = lax.rem(me - d + n, n)
        pltpu.make_async_remote_copy(
            src_ref=buf.at[src], dst_ref=buf.at[src], send_sem=send_sem.at[d - 1], recv_sem=recv_sem.at[d - 1],
            device_id={"tp": src}, device_id_type=MESH).wait_recv()
    return outs


def dense_kernel(n, cuts, part_ref, res_ref, gain_ref, gate_hbm, up_hbm, down_hbm, h_ref,
                 gate, up, down, recv, chunks, y, act, parts, recv2, cols, wsem, s1, r1, s2, r2, s3, r3, s4, r4):
    me = lax.axis_index("tp")
    tokens, hidden = y.shape
    rows, cw = tokens // n, hidden // n
    loads = []
    for k, (src, dst) in enumerate(((gate_hbm, gate), (up_hbm, up), (down_hbm, down))):
        step = dst.shape[0] // cuts
        for q in range(cuts):
            loads.append(pltpu.make_async_copy(src.at[pl.ds(q * step, step)], dst.at[pl.ds(q * step, step)], wsem.at[k * cuts + q]))
    for c in loads:
        c.start()
    barrier = pltpu.get_barrier_semaphore()
    for d in range(1, n):
        pl.semaphore_signal(barrier, inc=1, device_id={"tp": lax.rem(me + d, n)}, device_id_type=MESH)
    pl.semaphore_wait(barrier, n - 1)

    total, sends = sum_tp(me, n, rows, part_ref, recv, s1, r1)
    chunks[me] = (res_ref[pl.ds(me * rows, rows), :].astype(F32) + total).astype(BF16)
    sends = sends + share(n, me, chunks, s2, r2)
    for i in range(n):
        y[i * rows:(i + 1) * rows, :] = chunks[i]

    a = rms_norm(y[...], gain_ref[0:1, :])
    for c in loads[:2 * cuts]:
        c.wait()
    width = act.shape[1]
    step = 768
    for lo in range(0, width, step):
        hi = min(width, lo + step)
        act[:, lo:hi] = (silu(dot(a, gate[:, lo:hi])) * dot(a, up[:, lo:hi])).astype(BF16)
    for c in loads[2 * cuts:]:
        c.wait()
    inward = []
    for d in ([2, 1, 3] if n == 4 else list(range(1, n))) + [0]:
        peer = lax.rem(me + d, n)
        parts[d] = dot(act[...], down[:, pl.ds(pl.multiple_of(peer * cw, cw), cw)])
        if d:
            c = pltpu.make_async_remote_copy(src_ref=parts.at[d], dst_ref=recv2.at[d - 1], send_sem=s3.at[d - 1], recv_sem=r3.at[d - 1],
                                             device_id={"tp": peer}, device_id_type=MESH)
            c.start()
            inward.append(c)
    total = parts[0]
    for c in inward:
        c.wait_recv()
    for d in range(1, n):
        total = total + recv2[d - 1]
    cols[me] = (y[:, pl.ds(pl.multiple_of(me * cw, cw), cw)].astype(F32) + total).astype(BF16)
    sends = sends + inward + share(n, me, cols, s4, r4)
    for i in range(n):
        h_ref[:, i * cw:(i + 1) * cw] = cols[i]
    for c in sends:
        c.wait_send()


def dense_mlp(n, cid, part, res, gain, gate, up, down):
    tokens, hidden = part.shape
    rows, cw = tokens // n, hidden // n
    cuts = 4
    hbm = pl.BlockSpec(memory_space=pl.ANY)
    sem = pltpu.SemaphoreType.DMA((n - 1,))
    return pl.pallas_call(
        functools.partial(dense_kernel, n, cuts),
        out_shape=jax.ShapeDtypeStruct((tokens, hidden), BF16),
        in_specs=[VMEM] * 3 + [hbm] * 3, out_specs=VMEM,
        scratch_shapes=[pltpu.VMEM(gate.shape, BF16), pltpu.VMEM(up.shape, BF16), pltpu.VMEM(down.shape, BF16),
                        pltpu.VMEM((n - 1, rows, hidden), F32), pltpu.VMEM((n, rows, hidden), BF16), pltpu.VMEM((tokens, hidden), BF16),
                        pltpu.VMEM((tokens, gate.shape[1]), BF16), pltpu.VMEM((n, tokens, cw), F32), pltpu.VMEM((n - 1, tokens, cw), F32),
                        pltpu.VMEM((n, tokens, cw), BF16), pltpu.SemaphoreType.DMA((3 * cuts,))] + [sem] * 8,
        compiler_params=pltpu.CompilerParams(collective_id=cid, has_side_effects=True, vmem_limit_bytes=62 << 20),
        name="dense_mlp",
    )(part, res, gain, gate, up, down)


def dispatch_kernel(nt, nx, part_ref, res_ref, gain_ref, mask_ref, y_ref, tok_ref, recv, s1, r1, sx, rx, sy, ry, sd, rd):
    t = lax.axis_index("tp")
    ep = lax.axis_index("ep")
    x, c = ep // PAIR, lax.rem(ep, PAIR)
    sib = {"ep": x * PAIR + 1 - c}
    rows = y_ref.shape[0]
    width = part_ref.shape[1]
    half = width // 2
    total_w = tok_ref.shape[-1]
    lo, hi = pl.ds(0, half), pl.ds(half, total_w - half)
    tp_peer = [lax.rem(t + d, nt) for d in range(1, nt)]
    tp_src = [lax.rem(t - d + nt, nt) for d in range(1, nt)]
    x_peer = [lax.rem(x + d, nx) for d in range(1, nx)]
    x_src = [lax.rem(x - d + nx, nx) for d in range(1, nx)]

    barrier = pltpu.get_barrier_semaphore()
    for p in tp_peer:
        pl.semaphore_signal(barrier, inc=1, device_id={"tp": p}, device_id_type=MESH)
    for p in x_peer:
        pl.semaphore_signal(barrier, inc=1, device_id={"ep": p * PAIR + c}, device_id_type=MESH)
    pl.semaphore_signal(barrier, inc=1, device_id=sib, device_id_type=MESH)
    pl.semaphore_wait(barrier, nt + nx - 1)

    total, first = sum_tp(t, nt, rows, part_ref, recv, s1, r1)
    y = (res_ref[pl.ds(t * rows, rows), :].astype(F32) + total).astype(BF16)
    y_ref[...] = y
    tok_ref[x, c, t, :, pl.ds(0, width)] = rms_norm(y, gain_ref[1:2, :])
    tok_ref[x, c, t, :, pl.ds(width, total_w - width)] = mask_ref[pl.ds(t * rows, rows), :]

    def rc(ref, ssem, rsem, dev):
        return pltpu.make_async_remote_copy(src_ref=ref, dst_ref=ref, send_sem=ssem, recv_sem=rsem,
                                            device_id=dev, device_id_type=MESH)

    def to_x(p):
        return {"ep": p * PAIR + c}

    sends = list(first)
    for d in range(1, nx):
        s = rc(tok_ref.at[x, c, t, :, lo], sx.at[0, d - 1], rx.at[0, d - 1], to_x(x_peer[d - 1]))
        s.start()
        sends.append(s)
    for d in range(1, nt):
        s = rc(tok_ref.at[x, c, t, :, hi], sy.at[0, d - 1], ry.at[0, d - 1], {"tp": tp_peer[d - 1]})
        s.start()
        sends.append(s)
    for d in range(1, nx):
        rc(tok_ref.at[x_src[d - 1], c, t, :, lo], sx.at[0, d - 1], rx.at[0, d - 1], to_x(x_src[d - 1])).wait_recv()
    for d in range(1, nt):
        s = rc(tok_ref.at[:, c, t, :, lo], sy.at[1, d - 1], ry.at[1, d - 1], {"tp": tp_peer[d - 1]})
        s.start()
        sends.append(s)
    s = rc(tok_ref.at[:, c, t, :, lo], sd.at[0], rd.at[0], sib)
    s.start()
    sends.append(s)
    for d in range(1, nt):
        rc(tok_ref.at[x, c, tp_src[d - 1], :, hi], sy.at[0, d - 1], ry.at[0, d - 1], {"tp": tp_src[d - 1]}).wait_recv()
    for d in range(1, nx):
        s = rc(tok_ref.at[x, c, :, :, hi], sx.at[1, d - 1], rx.at[1, d - 1], to_x(x_peer[d - 1]))
        s.start()
        sends.append(s)
    s = rc(tok_ref.at[x, c, :, :, hi], sd.at[1], rd.at[1], sib)
    s.start()
    sends.append(s)
    k = 2
    for d in range(1, nt):
        src = tp_src[d - 1]
        rc(tok_ref.at[:, c, src, :, lo], sy.at[1, d - 1], ry.at[1, d - 1], {"tp": src}).wait_recv()
        s = rc(tok_ref.at[:, c, src, :, lo], sd.at[k], rd.at[k], sib)
        s.start()
        sends.append(s)
        k += 1
    for d in range(1, nx):
        src = x_src[d - 1]
        rc(tok_ref.at[src, c, :, :, hi], sx.at[1, d - 1], rx.at[1, d - 1], to_x(src)).wait_recv()
        s = rc(tok_ref.at[src, c, :, :, hi], sd.at[k], rd.at[k], sib)
        s.start()
        sends.append(s)
        k += 1
    o = 1 - c
    rc(tok_ref.at[:, o, t, :, lo], sd.at[0], rd.at[0], sib).wait_recv()
    rc(tok_ref.at[x, o, :, :, hi], sd.at[1], rd.at[1], sib).wait_recv()
    k = 2
    for d in range(1, nt):
        rc(tok_ref.at[:, o, tp_src[d - 1], :, lo], sd.at[k], rd.at[k], sib).wait_recv()
        k += 1
    for d in range(1, nx):
        rc(tok_ref.at[x_src[d - 1], o, :, :, hi], sd.at[k], rd.at[k], sib).wait_recv()
        k += 1
    for s in sends:
        s.wait_send()


def dispatch(nt, nx, cid, part, res, gain, mask):
    tokens, width = part.shape
    rows = tokens // nt
    total_w = width + mask.shape[1]
    ndd = nt + nx
    return pl.pallas_call(
        functools.partial(dispatch_kernel, nt, nx),
        out_shape=[jax.ShapeDtypeStruct((rows, width), BF16),
                   jax.ShapeDtypeStruct((nx, PAIR, nt, rows, total_w), BF16)],
        in_specs=[VMEM] * 4, out_specs=[VMEM] * 2,
        scratch_shapes=[pltpu.VMEM((nt - 1, rows, width), F32),
                        pltpu.SemaphoreType.DMA((nt - 1,)), pltpu.SemaphoreType.DMA((nt - 1,)),
                        pltpu.SemaphoreType.DMA((2, nx - 1)), pltpu.SemaphoreType.DMA((2, nx - 1)),
                        pltpu.SemaphoreType.DMA((2, nt - 1)), pltpu.SemaphoreType.DMA((2, nt - 1)),
                        pltpu.SemaphoreType.DMA((ndd,)), pltpu.SemaphoreType.DMA((ndd,))],
        compiler_params=pltpu.CompilerParams(collective_id=cid, has_side_effects=True),
        name="dispatch_tokens",
    )(part, res, gain, mask)


def combine_kernel(nt, nx, part_ref, y_ref, out_ref, half_in, sums, ax, ay, bx, by, own, chunks,
                   sd, rd, sx, rx, sy, ry, so, ro):
    t = lax.axis_index("tp")
    ep = lax.axis_index("ep")
    x, c = ep // PAIR, lax.rem(ep, PAIR)
    o = 1 - c
    sib = {"ep": x * PAIR + o}
    rows, width = y_ref.shape
    half = width // 2
    lo, hi = pl.ds(0, half), pl.ds(half, half)
    tp_peer = [lax.rem(t + d, nt) for d in range(1, nt)]
    tp_src = [lax.rem(t - d + nt, nt) for d in range(1, nt)]
    x_peer = [lax.rem(x + d, nx) for d in range(1, nx)]

    barrier = pltpu.get_barrier_semaphore()
    for p in tp_peer:
        pl.semaphore_signal(barrier, inc=1, device_id={"tp": p}, device_id_type=MESH)
    for p in x_peer:
        pl.semaphore_signal(barrier, inc=1, device_id={"ep": p * PAIR + c}, device_id_type=MESH)
    pl.semaphore_signal(barrier, inc=1, device_id=sib, device_id_type=MESH)
    pl.semaphore_wait(barrier, nt + nx - 1)

    def rc(src, dst, ssem, rsem, dev):
        return pltpu.make_async_remote_copy(src_ref=src, dst_ref=dst, send_sem=ssem, recv_sem=rsem,
                                            device_id=dev, device_id_type=MESH)

    sends = []
    pair = []
    for i in range(nx):
        s = rc(part_ref.at[i, o], half_in.at[i], sd.at[i], rd.at[i], sib)
        s.start()
        pair.append(s)
    for i in range(nx):
        pair[i].wait_recv()
        sums[i] = part_ref[i, c] + half_in[i]
    stage1x, stage1y = [], []
    for d in range(1, nx):
        s = rc(sums.at[x_peer[d - 1], :, :, lo], ax.at[d - 1], sx.at[0, d - 1], rx.at[0, d - 1], {"ep": x_peer[d - 1] * PAIR + c})
        s.start()
        stage1x.append(s)
    for d in range(1, nt):
        s = rc(sums.at[:, tp_peer[d - 1], :, hi], ay.at[d - 1], sy.at[0, d - 1], ry.at[0, d - 1], {"tp": tp_peer[d - 1]})
        s.start()
        stage1y.append(s)
    for s in stage1x:
        s.wait_recv()
    low = sums[x, :, :, lo]
    for d in range(1, nx):
        low = low + ax[d - 1]
    bx[...] = low
    stage2 = []
    for d in range(1, nt):
        s = rc(bx.at[tp_peer[d - 1]], own.at[0, d - 1], sy.at[1, d - 1], ry.at[1, d - 1], {"tp": tp_peer[d - 1]})
        s.start()
        stage2.append(s)
    for s in stage1y:
        s.wait_recv()
    high = sums[:, t, :, hi]
    for d in range(1, nt):
        high = high + ay[d - 1]
    by[...] = high
    for d in range(1, nx):
        s = rc(by.at[x_peer[d - 1]], own.at[1, d - 1], sx.at[1, d - 1], rx.at[1, d - 1], {"ep": x_peer[d - 1] * PAIR + c})
        s.start()
        stage2.append(s)
    for s in stage2:
        s.wait_recv()
    low = bx[t] + y_ref[:, :half].astype(F32)
    for d in range(1, nt):
        low = low + own[0, d - 1]
    high = by[x] + y_ref[:, half:].astype(F32)
    for d in range(1, nx):
        high = high + own[1, d - 1]
    chunks[t, :, lo] = low.astype(BF16)
    chunks[t, :, hi] = high.astype(BF16)
    outs = []
    for d in range(1, nt):
        s = rc(chunks.at[t], chunks.at[t], so.at[d - 1], ro.at[d - 1], {"tp": tp_peer[d - 1]})
        s.start()
        outs.append(s)
    for d in range(1, nt):
        rc(chunks.at[tp_src[d - 1]], chunks.at[tp_src[d - 1]], so.at[d - 1], ro.at[d - 1], {"tp": tp_src[d - 1]}).wait_recv()
    for s in pair + stage1x + stage1y + stage2 + outs:
        s.wait_send()
    out_ref[...] = chunks[...]


def combine(nt, nx, cid, part, y):
    rows, width = y.shape
    half = width // 2
    return pl.pallas_call(
        functools.partial(combine_kernel, nt, nx),
        out_shape=jax.ShapeDtypeStruct((nt, rows, width), BF16),
        in_specs=[VMEM] * 2, out_specs=VMEM,
        scratch_shapes=[pltpu.VMEM((nx, nt, rows, width), F32), pltpu.VMEM((nx, nt, rows, width), F32),
                        pltpu.VMEM((nx - 1, nt, rows, half), F32), pltpu.VMEM((nt - 1, nx, rows, half), F32),
                        pltpu.VMEM((nt, rows, half), F32), pltpu.VMEM((nx, rows, half), F32),
                        pltpu.VMEM((2, max(nt, nx) - 1, rows, half), F32),
                        pltpu.VMEM((nt, rows, width), BF16),
                        pltpu.SemaphoreType.DMA((nx,)), pltpu.SemaphoreType.DMA((nx,)),
                        pltpu.SemaphoreType.DMA((2, nx - 1)), pltpu.SemaphoreType.DMA((2, nx - 1)),
                        pltpu.SemaphoreType.DMA((2, nt - 1)), pltpu.SemaphoreType.DMA((2, nt - 1)),
                        pltpu.SemaphoreType.DMA((nt - 1,)), pltpu.SemaphoreType.DMA((nt - 1,))],
        compiler_params=pltpu.CompilerParams(collective_id=cid, has_side_effects=True, vmem_limit_bytes=62 << 20),
        name="combine_experts",
    )(part, y)


def moe_kernel(n_exp, own, tok_ref, router_ref, gate_ref, up_ref, down_ref, sg_ref, su_ref, sd_ref, out_ref, comb, xt, chosen):
    i = pl.program_id(0)
    ep = lax.axis_index("ep")
    hidden = out_ref.shape[1]
    experts = router_ref.shape[0]
    cols = 512

    @pl.when(i == 0)
    def _():
        logits = dot_nt(tok_ref[:, :hidden], router_ref[...])
        mask = tok_ref[:, hidden:hidden + experts].astype(F32)
        e = jnp.exp(logits - jnp.max(logits, axis=-1, keepdims=True))
        comb[...] = e / jnp.sum(e, axis=-1, keepdims=True) * mask
        for j in range(0, hidden, cols):
            xt[j:j + cols, :] = tok_ref[:, j:j + cols].T
        out_ref[...] = jnp.zeros_like(out_ref)
        chosen[...] = jnp.sum(mask, axis=0, keepdims=True)

    lane1 = lax.broadcasted_iota(jnp.int32, chosen.shape, 1)
    routed = jnp.sum(jnp.where(lane1 == ep * n_exp + i, chosen[...], 0.0))

    @pl.when((i < n_exp) & (routed > 0))
    def _():
        a = xt[...]
        act = (silu(dot(gate_ref[0], a)) * dot(up_ref[0], a)).astype(BF16).T
        lane = lax.broadcasted_iota(jnp.int32, comb.shape, 1)
        w = jnp.sum(jnp.where(lane == ep * n_exp + i, comb[...], 0.0), axis=1, keepdims=True)
        for j in range(0, hidden, cols):
            out_ref[:, j:j + cols] += w * dot(act, down_ref[0, :, j:j + cols])

    @pl.when(i >= n_exp)
    def _():
        r = pl.ds(pl.multiple_of(ep * own, own), own)
        a = tok_ref[r, :hidden]
        act = (silu(dot_nt(a, sg_ref[...])) * dot_nt(a, su_ref[...])).astype(BF16)
        for j in range(0, hidden, cols):
            out_ref[r, j:j + cols] += dot(act, sd_ref[:, j:j + cols])


def moe(own, tok, router_t, gate_t, up_t, down, sg_t, su_t, sd):
    tokens = tok.shape[0]
    n_exp, width, hidden = gate_t.shape
    steps = sg_t.shape[0] // width
    ex = lambda i: (jnp.minimum(i, n_exp - 1), 0, 0)
    sh = lambda i: (jnp.maximum(i - n_exp, 0), 0)
    return pl.pallas_call(
        functools.partial(moe_kernel, n_exp, own),
        grid=(n_exp + steps,),
        out_shape=jax.ShapeDtypeStruct((tokens, hidden), F32),
        in_specs=[pl.BlockSpec(tok.shape, lambda i: (0, 0)), pl.BlockSpec(router_t.shape, lambda i: (0, 0)),
                  pl.BlockSpec((1, width, hidden), ex), pl.BlockSpec((1, width, hidden), ex),
                  pl.BlockSpec((1, width, hidden), ex),
                  pl.BlockSpec((width, hidden), sh), pl.BlockSpec((width, hidden), sh), pl.BlockSpec((width, hidden), sh)],
        out_specs=pl.BlockSpec((tokens, hidden), lambda i: (0, 0)),
        scratch_shapes=[pltpu.VMEM((tokens, router_t.shape[0]), F32), pltpu.VMEM((hidden, tokens), BF16),
                        pltpu.VMEM((1, router_t.shape[0]), F32)],
        compiler_params=pltpu.CompilerParams(vmem_limit_bytes=62 << 20),
        name="moe_experts",
    )(tok, router_t, gate_t, up_t, down, sg_t, su_t, sd)


def rope_table(position, rope_dim):
    half_dim = rope_dim // 2
    inv_freq = ROPE_THETA ** (-(jnp.arange(half_dim, dtype=F32) * 2.0 / rope_dim))
    angles = position.astype(F32)[:, None] * inv_freq[None, :]
    return jnp.concatenate([jnp.cos(angles), jnp.sin(angles)], axis=1)


def attention_kernel(layer, group, pos_ref, h_ref, gain_ref, table_ref, gkv_ref, wq_ref, wkv_ref, wuk_ref,
                     lat_ref, rope_ref, wuv_hbm, wo_hbm, *rest):
    part_ref, lat_out, rope_out, qn, q1, q2, latn, ropet, o, wuv, wo, sem = rest[-12:]
    i = pl.program_id(0)
    seqs, sh, lora = qn.shape
    heads, qk = wq_ref.shape[1:3]
    steps = sh // heads
    nope = wuk_ref.shape[3]
    rope = qk - nope
    rh = rope // 2
    slots = lat_ref.shape[2]
    uv_copy = pltpu.make_async_copy(wuv_hbm.at[layer], wuv, sem.at[0])
    o_copy = pltpu.make_async_copy(wo_hbm.at[layer], wo, sem.at[1])

    @pl.when(i == 0)
    def _():
        uv_copy.start()
        o_copy.start()
        a = rms_norm(h_ref[...], gain_ref[layer:layer + 1, :])
        table = table_ref[...]
        cos_t, sin_t = table[:, :rh], table[:, rh:]
        for k in range(heads):
            qh = dot_nt(a, wq_ref[0, k, :nope, :]).astype(BF16)
            ql = dot_nt(qh, wuk_ref[0, k]).astype(BF16).astype(F32)
            x1 = dot_nt(a, wq_ref[0, k, nope:nope + rh, :])
            x2 = dot_nt(a, wq_ref[0, k, nope + rh:, :])
            r1 = (x1 * cos_t - x2 * sin_t).astype(BF16).astype(F32)
            r2 = (x2 * cos_t + x1 * sin_t).astype(BF16).astype(F32)
            for s in range(steps):
                rows = slice(s * seqs, (s + 1) * seqs)
                qn[:, s * heads + k, :] = ql[rows]
                q1[:, s * heads + k, :] = r1[rows]
                q2[:, s * heads + k, :] = r2[rows]
        latn[...] = rms_norm(dot_nt(a, wkv_ref[0, :lora, :]), gkv_ref[layer:layer + 1, :]).astype(F32)
        y1 = dot_nt(wkv_ref[0, lora:lora + rh, :], a)
        y2 = dot_nt(wkv_ref[0, lora + rh:, :], a)
        flip = table.T
        ct, st = flip[:rh, :], flip[rh:, :]
        ropet[:rh, :] = (y1 * ct - y2 * st).astype(BF16)
        ropet[rh:, :] = (y2 * ct + y1 * st).astype(BF16)

    tokens = latn.shape[0]
    tok_i = lax.broadcasted_iota(jnp.int32, (tokens, slots), 0)
    slot_i = lax.broadcasted_iota(jnp.int32, (tokens, slots), 1)
    lane = lax.broadcasted_iota(jnp.int32, (rope, slots), 1)
    row16 = lax.broadcasted_iota(jnp.int32, (16, 1), 0)
    slot_q = lax.broadcasted_iota(jnp.int32, (sh, slots), 1)
    step_q = lax.broadcasted_iota(jnp.int32, (sh, slots), 0) // heads
    keys, ropes, scores = [], [], []
    for j in range(group):
        b = i * group + j
        p = pos_ref[b]
        lat_out[0, j] = lat_ref[0, j]
        hot = jnp.zeros((tokens, slots), jnp.bool_)
        hit = jnp.zeros((rope, slots), jnp.bool_)
        for s in range(steps):
            base = pl.multiple_of((p + s) // 16 * 16, 16)
            blk = lat_out[0, j, pl.ds(base, 16), :].astype(F32)
            new = latn[pl.ds(s * seqs + b, 1), :]
            lat_out[0, j, pl.ds(base, 16), :] = jnp.where(row16 + base == p + s, new, blk).astype(BF16)
            hot = hot | ((tok_i == s * seqs + b) & (slot_i == p + s))
            hit = hit | (lane == p + s)
        upd = dot(ropet[...], hot.astype(F32).astype(BF16))
        rope_out[0, j] = jnp.where(hit, upd, rope_ref[0, j].astype(F32)).astype(BF16)
    for j in range(group):
        b = i * group + j
        sc = dot_nt(qn[b].astype(BF16), lat_out[0, j])
        sc = sc + dot(q1[b].astype(BF16), rope_out[0, j, :rh, :]) + dot(q2[b].astype(BF16), rope_out[0, j, rh:, :])
        sc = sc * (1.0 / math.sqrt(qk))
        scores.append(jnp.where(slot_q <= pos_ref[b] + step_q, sc, -1e30))
    for j in range(group):
        e = jnp.exp(scores[j] - jnp.max(scores[j], axis=-1, keepdims=True))
        scores[j] = (e / jnp.sum(e, axis=-1, keepdims=True)).astype(BF16)
    for j in range(group):
        o[i * group + j] = dot(scores[j], lat_out[0, j]).astype(BF16).astype(F32)

    @pl.when(i == pl.num_programs(0) - 1)
    def _():
        uv_copy.wait()
        o_copy.wait()
        outs = []
        for k in range(heads):
            oh = jnp.concatenate([o[:, s * heads + k, :] for s in range(steps)], axis=0).astype(BF16)
            outs.append(dot(oh, wuv[k]).astype(BF16))
        part_ref[...] = dot(jnp.concatenate(outs, axis=1), wo[...])


def attention(layer, hidden, pos, table, lat, rope_t, written, g_attn, wq_t, wkv_t, g_kv, wuk, wuv, w_o):
    tokens, width = hidden.shape
    seqs = pos.shape[0]
    heads, qk = wq_t.shape[1:3]
    slots, lora = lat.shape[2:]
    rope = rope_t.shape[2]
    sh = tokens // seqs * heads
    group = 8
    full = lambda shape: pl.BlockSpec(shape, lambda i, p: (0,) * len(shape))
    of_layer = lambda shape: pl.BlockSpec((1,) + shape, lambda i, p: (layer,) + (0,) * len(shape))
    lat_spec = pl.BlockSpec((1, group, slots, lora), lambda i, p: (layer, i, 0, 0))
    rope_spec = pl.BlockSpec((1, group, rope, slots), lambda i, p: (layer, i, 0, 0))
    hbm = pl.BlockSpec(memory_space=pl.ANY)
    operands = [pos, hidden, g_attn, table, g_kv, wq_t, wkv_t, wuk, lat, rope_t, wuv, w_o, *written]
    small = [full(x.shape) for x in operands[1:5]]
    return pl.pallas_call(
        functools.partial(attention_kernel, layer, group),
        grid_spec=pltpu.PrefetchScalarGridSpec(
            num_scalar_prefetch=1, grid=(seqs // group,),
            in_specs=small + [of_layer(wq_t.shape[1:]), of_layer(wkv_t.shape[1:]), of_layer(wuk.shape[1:]), lat_spec, rope_spec] + [hbm] * (2 + len(written)),
            out_specs=[full((tokens, width)), lat_spec, rope_spec],
            scratch_shapes=[pltpu.VMEM((seqs, sh, lora), F32), pltpu.VMEM((seqs, sh, rope // 2), F32), pltpu.VMEM((seqs, sh, rope // 2), F32),
                            pltpu.VMEM((tokens, lora), F32), pltpu.VMEM((rope, tokens), BF16), pltpu.VMEM((seqs, sh, lora), F32),
                            pltpu.VMEM(wuv.shape[1:], BF16), pltpu.VMEM(w_o.shape[1:], BF16), pltpu.SemaphoreType.DMA((2,))]),
        out_shape=[jax.ShapeDtypeStruct((tokens, width), F32), jax.ShapeDtypeStruct(lat.shape, BF16), jax.ShapeDtypeStruct(rope_t.shape, BF16)],
        input_output_aliases={12: 1, 13: 2} if written else {},
        compiler_params=pltpu.CompilerParams(vmem_limit_bytes=62 << 20),
        name="attention",
    )(*operands)


def solution(mesh):
    tok_axes = ('dp', 'ep')
    nt = mesh.shape['tp']
    nx = mesh.shape['ep'] // PAIR

    def device_fn(emb, pos, route_ids, lat_cache, rope_cache, attn_norm, w_q, w_dkv, kv_norm, w_uk, w_uv, w_o, mlp_norm, dense_gate, dense_up, dense_down, router, shared_gate, shared_up, shared_down, expert_gate, expert_up, expert_down):
        steps, seqs, hidden = emb.shape
        own = steps * seqs
        experts = router.shape[1]
        cur = jnp.concatenate([pos + s for s in range(steps)])
        table = rope_table(cur, rope_cache.shape[-1])
        ids = route_ids.reshape(own, -1)
        lanes = -(-experts // 128) * 128
        mask = jnp.any(ids[:, :, None] == jnp.arange(lanes)[None, None, :], axis=1).astype(BF16)

        h = emb.reshape(own, hidden)
        wq_t, wkv_t = w_q.transpose(0, 2, 3, 1), w_dkv.transpose(0, 2, 1)
        uk, uv = w_uk.transpose(0, 2, 1, 3), w_uv.transpose(0, 2, 1, 3)
        rope_t = rope_cache.transpose(0, 1, 3, 2)
        attend = lambda layer, x, *written: attention(layer, x, pos, table, lat_cache, rope_t, written, attn_norm, wq_t, wkv_t, kv_norm, uk, uv, w_o)
        part, lat, rop = attend(0, h)
        h = dense_mlp(nt, 0, part, h, mlp_norm, dense_gate, dense_up, dense_down)
        part, lat, rop = attend(1, h, lat, rop)
        y, tok = dispatch(nt, nx, 1, part, h, mlp_norm, mask)
        part = moe(own, tok.reshape(-1, tok.shape[-1]), router.T, expert_gate.transpose(0, 2, 1), expert_up.transpose(0, 2, 1), expert_down, shared_gate.T, shared_up.T, shared_down)
        out = combine(nt, nx, 2, part.reshape(nx, PAIR, nt, own // nt, hidden), y)
        return out.reshape(steps, seqs, hidden), lat, rop.transpose(0, 1, 3, 2)

    in_specs = (P(None, tok_axes, None), P(tok_axes), P(None, tok_axes, None), P(None, tok_axes, None, None), P(None, tok_axes, None, None), P(), P(None, None, 'tp', None), P(), P(), P(None, None, 'tp', None), P(None, None, 'tp', None), P(None, 'tp', None), P(), P(None, 'tp'), P(None, 'tp'), P('tp', None), P(), P(None, 'tp'), P(None, 'tp'), P('tp', None), P('ep', None, 'tp'), P('ep', None, 'tp'), P('ep', 'tp', None))
    out_specs = (P(None, tok_axes, None), P(None, tok_axes, None, None), P(None, tok_axes, None, None))
    return jax.shard_map(device_fn, mesh=mesh, in_specs=in_specs, out_specs=out_specs, check_vma=False)
```

```python
import functools
import math

import jax
import jax.numpy as jnp
from jax import lax
from jax.experimental import pallas as pl
from jax.experimental.pallas import tpu as pltpu
from jax.sharding import PartitionSpec as P

NORM_EPS = 1e-6
ROPE_THETA = 10000.0
F32 = jnp.float32
BF16 = jnp.bfloat16
MESH = pl.DeviceIdType.MESH
VMEM = pl.BlockSpec(memory_space=pltpu.VMEM)
NT = (((1,), (1,)), ((), ()))
PAIR = 2


def rms_norm(values, gain):
    wide = values.astype(F32)
    mean_sq = jnp.mean(wide * wide, axis=-1, keepdims=True)
    return (wide * lax.rsqrt(mean_sq + NORM_EPS) * gain).astype(BF16)


def silu(x):
    return x * jax.nn.sigmoid(x)


def dot(a, b):
    return jnp.dot(a, b, preferred_element_type=F32)


def dot_nt(a, b):
    return lax.dot_general(a, b, NT, preferred_element_type=F32)


def sum_tp(me, n, rows, part_ref, recv, send_sem, recv_sem):
    copies = []
    for d in [2, 1, 3] if n == 4 else range(1, n):
        peer = lax.rem(me + d, n)
        copies.append(pltpu.make_async_remote_copy(
            src_ref=part_ref.at[pl.ds(peer * rows, rows)], dst_ref=recv.at[d - 1],
            send_sem=send_sem.at[d - 1], recv_sem=recv_sem.at[d - 1],
            device_id={"tp": peer}, device_id_type=MESH))
    for c in copies:
        c.start()
    total = part_ref[pl.ds(me * rows, rows), :]
    for c in copies:
        c.wait_recv()
    for d in range(1, n):
        total = total + recv[d - 1]
    return total, copies


def share(n, me, buf, send_sem, recv_sem):
    outs = []
    for d in range(1, n):
        outs.append(pltpu.make_async_remote_copy(
            src_ref=buf.at[me], dst_ref=buf.at[me], send_sem=send_sem.at[d - 1], recv_sem=recv_sem.at[d - 1],
            device_id={"tp": lax.rem(me + d, n)}, device_id_type=MESH))
    for c in outs:
        c.start()
    for d in range(1, n):
        src = lax.rem(me - d + n, n)
        pltpu.make_async_remote_copy(
            src_ref=buf.at[src], dst_ref=buf.at[src], send_sem=send_sem.at[d - 1], recv_sem=recv_sem.at[d - 1],
            device_id={"tp": src}, device_id_type=MESH).wait_recv()
    return outs


def dense_kernel(n, cuts, part_ref, res_ref, gain_ref, gate_hbm, up_hbm, down_hbm, h_ref,
                 gate, up, down, recv, chunks, y, act, parts, recv2, cols, wsem, s1, r1, s2, r2, s3, r3, s4, r4):
    me = lax.axis_index("tp")
    tokens, hidden = y.shape
    rows, cw = tokens // n, hidden // n
    loads = []
    for k, (src, dst) in enumerate(((gate_hbm, gate), (up_hbm, up), (down_hbm, down))):
        step = dst.shape[0] // cuts
        for q in range(cuts):
            loads.append(pltpu.make_async_copy(src.at[pl.ds(q * step, step)], dst.at[pl.ds(q * step, step)], wsem.at[k * cuts + q]))
    for c in loads:
        c.start()
    barrier = pltpu.get_barrier_semaphore()
    for d in range(1, n):
        pl.semaphore_signal(barrier, inc=1, device_id={"tp": lax.rem(me + d, n)}, device_id_type=MESH)
    pl.semaphore_wait(barrier, n - 1)

    total, sends = sum_tp(me, n, rows, part_ref, recv, s1, r1)
    chunks[me] = (res_ref[pl.ds(me * rows, rows), :].astype(F32) + total).astype(BF16)
    sends = sends + share(n, me, chunks, s2, r2)
    for i in range(n):
        y[i * rows:(i + 1) * rows, :] = chunks[i]

    a = rms_norm(y[...], gain_ref[0:1, :])
    for c in loads[:2 * cuts]:
        c.wait()
    width = act.shape[1]
    step = 768
    for lo in range(0, width, step):
        hi = min(width, lo + step)
        act[:, lo:hi] = (silu(dot(a, gate[:, lo:hi])) * dot(a, up[:, lo:hi])).astype(BF16)
    for c in loads[2 * cuts:]:
        c.wait()
    inward = []
    for d in ([2, 1, 3] if n == 4 else list(range(1, n))) + [0]:
        peer = lax.rem(me + d, n)
        parts[d] = dot(act[...], down[:, pl.ds(pl.multiple_of(peer * cw, cw), cw)])
        if d:
            c = pltpu.make_async_remote_copy(src_ref=parts.at[d], dst_ref=recv2.at[d - 1], send_sem=s3.at[d - 1], recv_sem=r3.at[d - 1],
                                             device_id={"tp": peer}, device_id_type=MESH)
            c.start()
            inward.append(c)
    total = parts[0]
    for c in inward:
        c.wait_recv()
    for d in range(1, n):
        total = total + recv2[d - 1]
    cols[me] = (y[:, pl.ds(pl.multiple_of(me * cw, cw), cw)].astype(F32) + total).astype(BF16)
    sends = sends + inward + share(n, me, cols, s4, r4)
    for i in range(n):
        h_ref[:, i * cw:(i + 1) * cw] = cols[i]
    for c in sends:
        c.wait_send()


def dense_mlp(n, cid, part, res, gain, gate, up, down):
    tokens, hidden = part.shape
    rows, cw = tokens // n, hidden // n
    cuts = 4
    hbm = pl.BlockSpec(memory_space=pl.ANY)
    sem = pltpu.SemaphoreType.DMA((n - 1,))
    return pl.pallas_call(
        functools.partial(dense_kernel, n, cuts),
        out_shape=jax.ShapeDtypeStruct((tokens, hidden), BF16),
        in_specs=[VMEM] * 3 + [hbm] * 3, out_specs=VMEM,
        scratch_shapes=[pltpu.VMEM(gate.shape, BF16), pltpu.VMEM(up.shape, BF16), pltpu.VMEM(down.shape, BF16),
                        pltpu.VMEM((n - 1, rows, hidden), F32), pltpu.VMEM((n, rows, hidden), BF16), pltpu.VMEM((tokens, hidden), BF16),
                        pltpu.VMEM((tokens, gate.shape[1]), BF16), pltpu.VMEM((n, tokens, cw), F32), pltpu.VMEM((n - 1, tokens, cw), F32),
                        pltpu.VMEM((n, tokens, cw), BF16), pltpu.SemaphoreType.DMA((3 * cuts,))] + [sem] * 8,
        compiler_params=pltpu.CompilerParams(collective_id=cid, has_side_effects=True, vmem_limit_bytes=62 << 20),
        name="dense_mlp",
    )(part, res, gain, gate, up, down)


def routed_kernel(nt, nx, chunks, part_ref, res_ref, gain_ref, mask_ref, router_ref, gate_hbm, up_hbm, down_hbm, sg_hbm, su_hbm, sd_hbm, out_ref,
                  gate, up, down, sg, su, sd, tok, xt, act, comb_t, comb, sh, recv, y, po, pc, hin, ax, ay, bx, by, ox, oy, fin, wsem, shsem,
                  s1, r1, sx, rx, sy, ry, syl, ryl, sxh, rxh, sdd, rdd,
                  sp, rp, sx1, rx1, sy1, ry1, sy2, ry2, sx2, rx2, sag, rag):
    t = lax.axis_index("tp")
    ep = lax.axis_index("ep")
    x, c = ep // PAIR, lax.rem(ep, PAIR)
    o = 1 - c
    sib = {"ep": x * PAIR + o}
    rows, hidden = y.shape
    n_exp = gate.shape[0]
    experts = router_ref.shape[0]
    own = nt * rows
    side = nx * own
    total_w = tok.shape[-1]
    half = hidden // 2
    lo, hi = pl.ds(0, half), pl.ds(half, total_w - half)
    tps = range(nt - 1)
    xs = range(nx - 1)
    tp_peer = [lax.rem(t + d + 1, nt) for d in tps]
    tp_src = [lax.rem(t - d - 1 + nt, nt) for d in tps]
    x_peer = [lax.rem(x + d + 1, nx) for d in xs]
    x_src = [lax.rem(x - d - 1 + nx, nx) for d in xs]

    def to_x(p):
        return {"ep": p * PAIR + c}

    def to_t(p):
        return {"tp": p}

    def rc(src, dst, ssem, rsem, dev):
        return pltpu.make_async_remote_copy(src_ref=src, dst_ref=dst, send_sem=ssem, recv_sem=rsem, device_id=dev, device_id_type=MESH)

    sends = []

    def send(src, dst, ssem, rsem, dev):
        copy = rc(src, dst, ssem, rsem, dev)
        copy.start()
        sends.append(copy)
        return copy

    def arrived(ref, ssem, rsem, dev):
        rc(ref, ref, ssem, rsem, dev).wait_recv()

    shared_loads = [pltpu.make_async_copy(src, dst, shsem.at[k]) for k, (src, dst) in enumerate(((sg_hbm, sg), (su_hbm, su), (sd_hbm, sd)))]
    for copy in shared_loads:
        copy.start()
    weights = ((gate_hbm, gate), (up_hbm, up), (down_hbm, down))

    def load(k, e):
        return pltpu.make_async_copy(weights[k][0].at[e], weights[k][1].at[e], wsem.at[k, e])

    for e in range(n_exp):
        load(0, e).start()
        load(1, e).start()
    for e in range(n_exp):
        load(2, e).start()

    barrier = pltpu.get_barrier_semaphore()
    for p in tp_peer:
        pl.semaphore_signal(barrier, inc=1, device_id=to_t(p), device_id_type=MESH)
    for p in x_peer:
        pl.semaphore_signal(barrier, inc=1, device_id=to_x(p), device_id_type=MESH)
    pl.semaphore_signal(barrier, inc=1, device_id=sib, device_id_type=MESH)
    pl.semaphore_wait(barrier, nt + nx - 1)

    total, first = sum_tp(t, nt, rows, part_ref, recv, s1, r1)
    sends += first
    mine = (res_ref[pl.ds(t * rows, rows), :].astype(F32) + total).astype(BF16)
    y[...] = mine
    tok[c, x, t, :, pl.ds(0, hidden)] = rms_norm(mine, gain_ref[1:2, :])
    tok[c, x, t, :, pl.ds(hidden, total_w - hidden)] = mask_ref[pl.ds(t * rows, rows), :]
    row = tok.at[c, x, t]
    for d in xs:
        send(row, row, sx.at[d], rx.at[d], to_x(x_peer[d]))
    for d in tps:
        send(row, row, sy.at[d], ry.at[d], to_t(tp_peer[d]))
    send(row, row, sdd.at[0], rdd.at[0], sib)
    k = 1
    passed = []
    for d in xs:
        ref = tok.at[c, x_src[d], t]
        arrived(ref, sx.at[d], rx.at[d], to_x(x_src[d]))
        low = tok.at[c, x_src[d], t, :, lo]
        for f in tps:
            send(low, low, syl.at[d, f], ryl.at[d, f], to_t(tp_peer[f]))
        send(ref, ref, sdd.at[k], rdd.at[k], sib)
        passed.append((x_src[d], t, None))
        k += 1
    for d in tps:
        ref = tok.at[c, x, tp_src[d]]
        arrived(ref, sy.at[d], ry.at[d], to_t(tp_src[d]))
        high = tok.at[c, x, tp_src[d], :, hi]
        for f in xs:
            send(high, high, sxh.at[d, f], rxh.at[d, f], to_x(x_peer[f]))
        send(ref, ref, sdd.at[k], rdd.at[k], sib)
        passed.append((x, tp_src[d], None))
        k += 1

    for copy in shared_loads:
        copy.wait()
    a = tok[c, x, :, :, :hidden].reshape(own, hidden)
    mid = (silu(dot_nt(a, sg[...])) * dot_nt(a, su[...])).astype(BF16)
    cw = hidden // chunks
    for j in range(chunks):
        sh[:, :, j * cw:(j + 1) * cw] = dot(mid, sd[:, j * cw:(j + 1) * cw]).reshape(nt, rows, cw)

    for d in xs:
        for f in tps:
            ref = tok.at[c, x_src[d], tp_src[f], :, lo]
            arrived(ref, syl.at[d, f], ryl.at[d, f], to_t(tp_src[f]))
            send(ref, ref, sdd.at[k], rdd.at[k], sib)
            passed.append((x_src[d], tp_src[f], lo))
            k += 1
    for d in tps:
        for f in xs:
            ref = tok.at[c, x_src[f], tp_src[d], :, hi]
            arrived(ref, sxh.at[d, f], rxh.at[d, f], to_x(x_src[f]))
            send(ref, ref, sdd.at[k], rdd.at[k], sib)
            passed.append((x_src[f], tp_src[d], hi))
            k += 1
    ref = tok.at[o, x, t]
    arrived(ref, sdd.at[0], rdd.at[0], sib)
    for k, (i, q, cols) in enumerate(passed):
        ref = tok.at[o, i, q] if cols is None else tok.at[o, i, q, :, cols]
        arrived(ref, sdd.at[k + 1], rdd.at[k + 1], sib)

    lanes = 2 * own
    for q in range(PAIR):
        for i in range(0, nx, 2):
            for j in range(0, hidden, 512):
                xt[j:j + 512, q * side + i * own:q * side + i * own + lanes] = tok[q, i:i + 2, :, :, j:j + 512].reshape(lanes, 512).T
            comb_t[:, q * side + i * own:q * side + i * own + lanes] = tok[q, i:i + 2, :, :, hidden:].reshape(lanes, total_w - hidden).astype(F32).T
    logits = dot(router_ref[...], xt[...])
    e = jnp.exp(logits - jnp.max(logits, axis=0, keepdims=True))
    comb_t[:experts, :] = e / jnp.sum(e, axis=0, keepdims=True) * comb_t[:experts, :]
    comb[...] = comb_t[pl.ds(pl.multiple_of(ep * n_exp, n_exp), n_exp), :].T

    def gate_up(e, carry):
        load(0, e).wait()
        load(1, e).wait()
        for q in range(PAIR):
            cols = xt[:, q * side:(q + 1) * side]
            act[e, q * side:(q + 1) * side, :] = (silu(dot(gate[e], cols)) * dot(up[e], cols)).astype(BF16).T
        return carry

    lax.fori_loop(0, n_exp, gate_up, 0)
    for e in range(n_exp):
        load(2, e).wait()

    hw = cw // 2
    left, right = pl.ds(0, hw), pl.ds(hw, hw)

    def expert_sum(q, j, dst, b):
        r = pl.ds(pl.multiple_of(q * side, side), side)
        w = comb[r, :]
        for e in range(n_exp):
            v = (w[:, e:e + 1] * dot(act[e, r, :], down[e, :, j * cw:(j + 1) * cw])).reshape(nx, nt, rows, cw)
            dst[b] = v if e == 0 else dst[b] + v

    pair_sends = {}
    stage1 = {}
    stage2 = {}

    def other_side(j):
        if j >= 2:
            pair_sends[j - 2].wait_send()
        expert_sum(o, j, po, j % 2)
        copy = rc(po.at[j % 2], hin.at[j], sp.at[j], rp.at[j], sib)
        copy.start()
        pair_sends[j] = copy

    def own_side(j):
        expert_sum(c, j, pc, j % 2)

    def first_sums(j):
        pair_sends[j].wait_recv()
        for i in range(nx):
            hin[j, i] = hin[j, i] + pc[j % 2, i]
        hin[j, x] = hin[j, x] + sh[:, :, j * cw:(j + 1) * cw]
        stage1[j] = [send(hin.at[j, x_peer[d], :, :, left], ax.at[j, d], sx1.at[j, d], rx1.at[j, d], to_x(x_peer[d])) for d in xs] + [
            send(hin.at[j, :, tp_peer[d], :, right], ay.at[j, d], sy1.at[j, d], ry1.at[j, d], to_t(tp_peer[d])) for d in tps]

    def second_sums(j):
        for copy in stage1[j]:
            copy.wait_recv()
        v = hin[j, x, :, :, left]
        for d in xs:
            v = v + ax[j, d]
        bx[j] = v
        v = hin[j, :, t, :, right]
        for d in tps:
            v = v + ay[j, d]
        by[j] = v
        stage2[j] = [send(bx.at[j, tp_peer[d]], ox.at[j, d], sy2.at[j, d], ry2.at[j, d], to_t(tp_peer[d])) for d in tps] + [
            send(by.at[j, x_peer[d]], oy.at[j, d], sx2.at[j, d], rx2.at[j, d], to_x(x_peer[d])) for d in xs]

    def last_sums(j):
        for copy in stage2[j]:
            copy.wait_recv()
        v = bx[j, t] + y[:, j * cw:j * cw + hw].astype(F32)
        for d in tps:
            v = v + ox[j, d]
        fin[j, t, :, left] = v.astype(BF16)
        v = by[j, x] + y[:, j * cw + hw:(j + 1) * cw].astype(F32)
        for d in xs:
            v = v + oy[j, d]
        fin[j, t, :, right] = v.astype(BF16)
        for d in tps:
            send(fin.at[j, t], fin.at[j, t], sag.at[j, d], rag.at[j, d], to_t(tp_peer[d]))

    for j in range(chunks):
        other_side(j)
        if j:
            first_sums(j - 1)
        own_side(j)
    first_sums(chunks - 1)
    second_sums(0)
    for j in range(1, chunks):
        second_sums(j)
        last_sums(j - 1)
    last_sums(chunks - 1)
    for j in range(chunks):
        for d in tps:
            arrived(fin.at[j, tp_src[d]], sag.at[j, d], rag.at[j, d], to_t(tp_src[d]))
        out_ref[:, :, j * cw:(j + 1) * cw] = fin[j]
    for j in range(max(0, chunks - 2), chunks):
        pair_sends[j].wait_send()
    for copy in sends:
        copy.wait_send()


def routed(nt, nx, cid, part, res, gain, mask, router_t, gate_t, up_t, down, sg_t, su_t, sd):
    tokens, hidden = part.shape
    rows = tokens // nt
    n_exp = gate_t.shape[0]
    total_w = hidden + mask.shape[1]
    every = PAIR * nx * tokens
    chunks = 4
    cw = hidden // chunks
    hw = cw // 2
    hbm = pl.BlockSpec(memory_space=pl.ANY)
    sem = lambda *shape: [pltpu.SemaphoreType.DMA(shape)] * 2
    f32 = lambda *shape: pltpu.VMEM(shape, F32)
    bf16 = lambda *shape: pltpu.VMEM(shape, BF16)
    mx, mt = nx - 1, nt - 1
    return pl.pallas_call(
        functools.partial(routed_kernel, nt, nx, chunks),
        out_shape=jax.ShapeDtypeStruct((nt, rows, hidden), BF16),
        in_specs=[VMEM] * 5 + [hbm] * 6, out_specs=VMEM,
        scratch_shapes=[bf16(*gate_t.shape), bf16(*up_t.shape), bf16(*down.shape), bf16(*sg_t.shape), bf16(*su_t.shape), bf16(*sd.shape),
                        bf16(PAIR, nx, nt, rows, total_w), bf16(hidden, every), bf16(n_exp, every, down.shape[1]),
                        f32(mask.shape[1], every), f32(every, n_exp), f32(nt, rows, hidden), f32(mt, rows, hidden), bf16(rows, hidden),
                        f32(2, nx, nt, rows, cw), f32(2, nx, nt, rows, cw), f32(chunks, nx, nt, rows, cw),
                        f32(chunks, mx, nt, rows, hw), f32(chunks, mt, nx, rows, hw), f32(chunks, nt, rows, hw), f32(chunks, nx, rows, hw),
                        f32(chunks, mt, rows, hw), f32(chunks, mx, rows, hw), bf16(chunks, nt, rows, cw),
                        pltpu.SemaphoreType.DMA((3, n_exp)), pltpu.SemaphoreType.DMA((3,))]
        + sem(mt) + sem(mx) + sem(mt) + sem(mx, mt) + sem(mt, mx) + sem(1 + mx + mt + 2 * mx * mt)
        + sem(chunks) + sem(chunks, mx) + sem(chunks, mt) + sem(chunks, mt) + sem(chunks, mx) + sem(chunks, mt),
        compiler_params=pltpu.CompilerParams(collective_id=cid, has_side_effects=True, vmem_limit_bytes=67_000_000),
        name="routed_layer",
    )(part, res, gain, mask, router_t, gate_t, up_t, down, sg_t, su_t, sd)


def rope_table(position, rope_dim):
    half_dim = rope_dim // 2
    inv_freq = ROPE_THETA ** (-(jnp.arange(half_dim, dtype=F32) * 2.0 / rope_dim))
    angles = position.astype(F32)[:, None] * inv_freq[None, :]
    return jnp.concatenate([jnp.cos(angles), jnp.sin(angles)], axis=1)


def attention_kernel(layer, group, pos_ref, h_ref, gain_ref, table_ref, gkv_ref, wq_ref, wkv_ref, wuk_ref,
                     lat_ref, rope_ref, wuv_hbm, wo_hbm, *rest):
    part_ref, lat_out, rope_out, qn, q1, q2, latn, ropet, o, wuv, wo, sem = rest[-12:]
    i = pl.program_id(0)
    seqs, sh, lora = qn.shape
    heads, qk = wq_ref.shape[1:3]
    steps = sh // heads
    nope = wuk_ref.shape[3]
    rope = qk - nope
    rh = rope // 2
    slots = lat_ref.shape[2]
    uv_copy = pltpu.make_async_copy(wuv_hbm.at[layer], wuv, sem.at[0])
    o_copy = pltpu.make_async_copy(wo_hbm.at[layer], wo, sem.at[1])

    @pl.when(i == 0)
    def _():
        uv_copy.start()
        o_copy.start()
        a = rms_norm(h_ref[...], gain_ref[layer:layer + 1, :])
        table = table_ref[...]
        cos_t, sin_t = table[:, :rh], table[:, rh:]
        for k in range(heads):
            qh = dot_nt(a, wq_ref[0, k, :nope, :]).astype(BF16)
            ql = dot_nt(qh, wuk_ref[0, k]).astype(BF16).astype(F32)
            x1 = dot_nt(a, wq_ref[0, k, nope:nope + rh, :])
            x2 = dot_nt(a, wq_ref[0, k, nope + rh:, :])
            r1 = (x1 * cos_t - x2 * sin_t).astype(BF16).astype(F32)
            r2 = (x2 * cos_t + x1 * sin_t).astype(BF16).astype(F32)
            for s in range(steps):
                rows = slice(s * seqs, (s + 1) * seqs)
                qn[:, s * heads + k, :] = ql[rows]
                q1[:, s * heads + k, :] = r1[rows]
                q2[:, s * heads + k, :] = r2[rows]
        latn[...] = rms_norm(dot_nt(a, wkv_ref[0, :lora, :]), gkv_ref[layer:layer + 1, :]).astype(F32)
        y1 = dot_nt(wkv_ref[0, lora:lora + rh, :], a)
        y2 = dot_nt(wkv_ref[0, lora + rh:, :], a)
        flip = table.T
        ct, st = flip[:rh, :], flip[rh:, :]
        ropet[:rh, :] = (y1 * ct - y2 * st).astype(BF16)
        ropet[rh:, :] = (y2 * ct + y1 * st).astype(BF16)

    tokens = latn.shape[0]
    tok_i = lax.broadcasted_iota(jnp.int32, (tokens, slots), 0)
    slot_i = lax.broadcasted_iota(jnp.int32, (tokens, slots), 1)
    lane = lax.broadcasted_iota(jnp.int32, (rope, slots), 1)
    row16 = lax.broadcasted_iota(jnp.int32, (16, 1), 0)
    slot_q = lax.broadcasted_iota(jnp.int32, (sh, slots), 1)
    step_q = lax.broadcasted_iota(jnp.int32, (sh, slots), 0) // heads
    keys, ropes, scores = [], [], []
    for j in range(group):
        b = i * group + j
        p = pos_ref[b]
        lat_out[0, j] = lat_ref[0, j]
        hot = jnp.zeros((tokens, slots), jnp.bool_)
        hit = jnp.zeros((rope, slots), jnp.bool_)
        for s in range(steps):
            base = pl.multiple_of((p + s) // 16 * 16, 16)
            blk = lat_out[0, j, pl.ds(base, 16), :].astype(F32)
            new = latn[pl.ds(s * seqs + b, 1), :]
            lat_out[0, j, pl.ds(base, 16), :] = jnp.where(row16 + base == p + s, new, blk).astype(BF16)
            hot = hot | ((tok_i == s * seqs + b) & (slot_i == p + s))
            hit = hit | (lane == p + s)
        upd = dot(ropet[...], hot.astype(F32).astype(BF16))
        rope_out[0, j] = jnp.where(hit, upd, rope_ref[0, j].astype(F32)).astype(BF16)
    for j in range(group):
        b = i * group + j
        sc = dot_nt(qn[b].astype(BF16), lat_out[0, j])
        sc = sc + dot(q1[b].astype(BF16), rope_out[0, j, :rh, :]) + dot(q2[b].astype(BF16), rope_out[0, j, rh:, :])
        sc = sc * (1.0 / math.sqrt(qk))
        scores.append(jnp.where(slot_q <= pos_ref[b] + step_q, sc, -1e30))
    for j in range(group):
        e = jnp.exp(scores[j] - jnp.max(scores[j], axis=-1, keepdims=True))
        scores[j] = (e / jnp.sum(e, axis=-1, keepdims=True)).astype(BF16)
    for j in range(group):
        o[i * group + j] = dot(scores[j], lat_out[0, j]).astype(BF16).astype(F32)

    @pl.when(i == pl.num_programs(0) - 1)
    def _():
        uv_copy.wait()
        o_copy.wait()
        outs = []
        for k in range(heads):
            oh = jnp.concatenate([o[:, s * heads + k, :] for s in range(steps)], axis=0).astype(BF16)
            outs.append(dot(oh, wuv[k]).astype(BF16))
        part_ref[...] = dot(jnp.concatenate(outs, axis=1), wo[...])


def attention(layer, hidden, pos, table, lat, rope_t, written, g_attn, wq_t, wkv_t, g_kv, wuk, wuv, w_o):
    tokens, width = hidden.shape
    seqs = pos.shape[0]
    heads, qk = wq_t.shape[1:3]
    slots, lora = lat.shape[2:]
    rope = rope_t.shape[2]
    sh = tokens // seqs * heads
    group = 8
    full = lambda shape: pl.BlockSpec(shape, lambda i, p: (0,) * len(shape))
    of_layer = lambda shape: pl.BlockSpec((1,) + shape, lambda i, p: (layer,) + (0,) * len(shape))
    lat_spec = pl.BlockSpec((1, group, slots, lora), lambda i, p: (layer, i, 0, 0))
    rope_spec = pl.BlockSpec((1, group, rope, slots), lambda i, p: (layer, i, 0, 0))
    hbm = pl.BlockSpec(memory_space=pl.ANY)
    operands = [pos, hidden, g_attn, table, g_kv, wq_t, wkv_t, wuk, lat, rope_t, wuv, w_o, *written]
    small = [full(x.shape) for x in operands[1:5]]
    return pl.pallas_call(
        functools.partial(attention_kernel, layer, group),
        grid_spec=pltpu.PrefetchScalarGridSpec(
            num_scalar_prefetch=1, grid=(seqs // group,),
            in_specs=small + [of_layer(wq_t.shape[1:]), of_layer(wkv_t.shape[1:]), of_layer(wuk.shape[1:]), lat_spec, rope_spec] + [hbm] * (2 + len(written)),
            out_specs=[full((tokens, width)), lat_spec, rope_spec],
            scratch_shapes=[pltpu.VMEM((seqs, sh, lora), F32), pltpu.VMEM((seqs, sh, rope // 2), F32), pltpu.VMEM((seqs, sh, rope // 2), F32),
                            pltpu.VMEM((tokens, lora), F32), pltpu.VMEM((rope, tokens), BF16), pltpu.VMEM((seqs, sh, lora), F32),
                            pltpu.VMEM(wuv.shape[1:], BF16), pltpu.VMEM(w_o.shape[1:], BF16), pltpu.SemaphoreType.DMA((2,))]),
        out_shape=[jax.ShapeDtypeStruct((tokens, width), F32), jax.ShapeDtypeStruct(lat.shape, BF16), jax.ShapeDtypeStruct(rope_t.shape, BF16)],
        input_output_aliases={12: 1, 13: 2} if written else {},
        compiler_params=pltpu.CompilerParams(vmem_limit_bytes=62 << 20),
        name="attention",
    )(*operands)


def solution(mesh):
    tok_axes = ('dp', 'ep')
    nt = mesh.shape['tp']
    nx = mesh.shape['ep'] // PAIR

    def device_fn(emb, pos, route_ids, lat_cache, rope_cache, attn_norm, w_q, w_dkv, kv_norm, w_uk, w_uv, w_o, mlp_norm, dense_gate, dense_up, dense_down, router, shared_gate, shared_up, shared_down, expert_gate, expert_up, expert_down):
        steps, seqs, hidden = emb.shape
        own = steps * seqs
        experts = router.shape[1]
        cur = jnp.concatenate([pos + s for s in range(steps)])
        table = rope_table(cur, rope_cache.shape[-1])
        ids = route_ids.reshape(own, -1)
        lanes = -(-experts // 128) * 128
        mask = jnp.any(ids[:, :, None] == jnp.arange(lanes)[None, None, :], axis=1).astype(BF16)

        h = emb.reshape(own, hidden)
        wq_t, wkv_t = w_q.transpose(0, 2, 3, 1), w_dkv.transpose(0, 2, 1)
        uk, uv = w_uk.transpose(0, 2, 1, 3), w_uv.transpose(0, 2, 1, 3)
        rope_t = rope_cache.transpose(0, 1, 3, 2)
        attend = lambda layer, x, *written: attention(layer, x, pos, table, lat_cache, rope_t, written, attn_norm, wq_t, wkv_t, kv_norm, uk, uv, w_o)
        part, lat, rop = attend(0, h)
        h = dense_mlp(nt, 0, part, h, mlp_norm, dense_gate, dense_up, dense_down)
        part, lat, rop = attend(1, h, lat, rop)
        out = routed(nt, nx, 1, part, h, mlp_norm, mask, router.T, expert_gate.transpose(0, 2, 1), expert_up.transpose(0, 2, 1), expert_down, shared_gate.T, shared_up.T, shared_down)
        return out.reshape(steps, seqs, hidden), lat, rop.transpose(0, 1, 3, 2)

    in_specs = (P(None, tok_axes, None), P(tok_axes), P(None, tok_axes, None), P(None, tok_axes, None, None), P(None, tok_axes, None, None), P(), P(None, None, 'tp', None), P(), P(), P(None, None, 'tp', None), P(None, None, 'tp', None), P(None, 'tp', None), P(), P(None, 'tp'), P(None, 'tp'), P('tp', None), P(), P(None, 'tp'), P(None, 'tp'), P('tp', None), P('ep', None, 'tp'), P('ep', None, 'tp'), P('ep', 'tp', None))
    out_specs = (P(None, tok_axes, None), P(None, tok_axes, None, None), P(None, tok_axes, None, None))
    return jax.shard_map(device_fn, mesh=mesh, in_specs=in_specs, out_specs=out_specs, check_vma=False)
```

```python
import functools
import math

import jax
import jax.numpy as jnp
import numpy as np
from jax import lax
from jax.experimental import pallas as pl
from jax.experimental.pallas import tpu as pltpu
from jax.sharding import PartitionSpec as P

NORM_EPS = 1e-6
ROPE_THETA = 10000.0
F32 = jnp.float32
BF16 = jnp.bfloat16
MESH = pl.DeviceIdType.MESH
VMEM = pl.BlockSpec(memory_space=pltpu.VMEM)
NT = (((1,), (1,)), ((), ()))
PAIR = 2


def rms_norm(values, gain):
    wide = values.astype(F32)
    mean_sq = jnp.mean(wide * wide, axis=-1, keepdims=True)
    return (wide * lax.rsqrt(mean_sq + NORM_EPS) * gain).astype(BF16)


def silu(x):
    return x * jax.nn.sigmoid(x)


def dot(a, b):
    return jnp.dot(a, b, preferred_element_type=F32)


def dot_nt(a, b):
    return lax.dot_general(a, b, NT, preferred_element_type=F32)


def ring4(me):
    return lax.rem(me, 2) * -2 + 1 + me, 3 - me, lax.rem(me + 2, 4)


def to_tp(p):
    return {"tp": p}


class Halving:
    def __init__(self, me, recv, snd, ssem, rsem):
        self.a, self.b, self.c = ring4(me)
        self.me, self.recv, self.snd, self.ssem, self.rsem = me, recv, snd, ssem, rsem
        self.copies = {}

    def put(self, k, src, peer):
        copy = pltpu.make_async_remote_copy(src_ref=src, dst_ref=self.recv.at[k], send_sem=self.ssem.at[k], recv_sem=self.rsem.at[k],
                                            device_id=to_tp(peer), device_id_type=MESH)
        copy.start()
        self.copies[k] = copy

    def far(self, piece):
        self.put(0, piece(self.c, 0), self.a)
        self.put(1, piece(self.c, 1), self.b)

    def near_a(self, piece):
        self.put(2, piece(self.a, 0), self.a)

    def near_b(self, piece):
        self.put(3, piece(self.b, 1), self.b)

    def relay(self, piece):
        self.copies[0].wait_recv()
        self.snd[0] = piece(self.b, 0)[...] + self.recv[0]
        self.put(4, self.snd.at[0], self.b)
        self.copies[1].wait_recv()
        self.snd[1] = piece(self.a, 1)[...] + self.recv[1]
        self.put(5, self.snd.at[1], self.a)

    def result(self, piece):
        out = []
        for h in range(2):
            self.copies[2 + h].wait_recv()
            self.copies[4 + h].wait_recv()
            out.append(piece(self.me, h)[...] + self.recv[2 + h] + self.recv[4 + h])
        return out


def sum_tp(me, n, rows, part_ref, recv, send_sem, recv_sem):
    copies = []
    for d in [2, 1, 3] if n == 4 else range(1, n):
        peer = lax.rem(me + d, n)
        copies.append(pltpu.make_async_remote_copy(
            src_ref=part_ref.at[pl.ds(pl.multiple_of(peer * rows, rows), rows)], dst_ref=recv.at[d - 1],
            send_sem=send_sem.at[d - 1], recv_sem=recv_sem.at[d - 1], device_id=to_tp(peer), device_id_type=MESH))
    for c in copies:
        c.start()
    total = part_ref[pl.ds(pl.multiple_of(me * rows, rows), rows), :]
    for c in copies:
        c.wait_recv()
    for d in range(1, n):
        total = total + recv[d - 1]
    return total, copies


def share(n, me, buf, send_sem, recv_sem):
    outs = []
    for d in range(1, n):
        outs.append(pltpu.make_async_remote_copy(
            src_ref=buf.at[me], dst_ref=buf.at[me], send_sem=send_sem.at[d - 1], recv_sem=recv_sem.at[d - 1],
            device_id={"tp": lax.rem(me + d, n)}, device_id_type=MESH))
    for c in outs:
        c.start()
    for d in range(1, n):
        src = lax.rem(me - d + n, n)
        pltpu.make_async_remote_copy(
            src_ref=buf.at[src], dst_ref=buf.at[src], send_sem=send_sem.at[d - 1], recv_sem=recv_sem.at[d - 1],
            device_id={"tp": src}, device_id_type=MESH).wait_recv()
    return outs


def dense_kernel(n, cuts, part_ref, res_ref, gain_ref, gate_hbm, up_hbm, down_hbm, h_ref,
                 gate, up, down, recv, chunks, y, act, parts, recv2, snd2, cols, wsem, s3, r3, s1, r1, s2, r2, s4, r4):
    me = lax.axis_index("tp")
    tokens, hidden = y.shape
    rows, cw = tokens // n, hidden // n
    loads = []
    for k, (src, dst) in enumerate(((gate_hbm, gate), (up_hbm, up), (down_hbm, down))):
        step = dst.shape[0] // cuts
        for q in range(cuts):
            loads.append(pltpu.make_async_copy(src.at[pl.ds(q * step, step)], dst.at[pl.ds(q * step, step)], wsem.at[k * cuts + q]))
    for c in loads:
        c.start()
    barrier = pltpu.get_barrier_semaphore()
    for d in range(1, n):
        pl.semaphore_signal(barrier, inc=1, device_id={"tp": lax.rem(me + d, n)}, device_id_type=MESH)
    pl.semaphore_wait(barrier, n - 1)

    total, sends = sum_tp(me, n, rows, part_ref, recv, s1, r1)
    chunks[me] = (res_ref[pl.ds(me * rows, rows), :].astype(F32) + total).astype(BF16)
    sends = sends + share(n, me, chunks, s2, r2)
    for i in range(n):
        y[i * rows:(i + 1) * rows, :] = chunks[i]

    a = rms_norm(y[...], gain_ref[0:1, :])
    for c in loads[:2 * cuts]:
        c.wait()
    width = act.shape[1]
    step = 768
    for lo in range(0, width, step):
        hi = min(width, lo + step)
        act[:, lo:hi] = (silu(dot(a, gate[:, lo:hi])) * dot(a, up[:, lo:hi])).astype(BF16)
    for c in loads[2 * cuts:]:
        c.wait()
    red = Halving(me, recv2, snd2, s3, r3)
    slot = [me, red.a, red.b, red.c]
    hr = tokens // 2

    def term(k):
        parts[k] = dot(act[...], down[:, pl.ds(pl.multiple_of(slot[k] * cw, cw), cw)])

    term(3)
    red.far(lambda owner, h: parts.at[3, pl.ds(h * hr, hr)])
    term(1)
    red.near_a(lambda owner, h: parts.at[1, pl.ds(h * hr, hr)])
    term(2)
    red.near_b(lambda owner, h: parts.at[2, pl.ds(h * hr, hr)])
    red.relay(lambda owner, h: parts.at[2 - h, pl.ds(h * hr, hr)])
    term(0)
    total = jnp.concatenate(red.result(lambda owner, h: parts.at[0, pl.ds(h * hr, hr)]), axis=0)
    cols[me] = (y[:, pl.ds(pl.multiple_of(me * cw, cw), cw)].astype(F32) + total).astype(BF16)
    sends = sends + list(red.copies.values()) + share(n, me, cols, s4, r4)
    for i in range(n):
        h_ref[:, i * cw:(i + 1) * cw] = cols[i]
    for c in sends:
        c.wait_send()


def dense_mlp(n, cid, part, res, gain, gate, up, down):
    tokens, hidden = part.shape
    rows, cw = tokens // n, hidden // n
    cuts = 4
    hbm = pl.BlockSpec(memory_space=pl.ANY)
    sem = pltpu.SemaphoreType.DMA((n - 1,))
    return pl.pallas_call(
        functools.partial(dense_kernel, n, cuts),
        out_shape=jax.ShapeDtypeStruct((tokens, hidden), BF16),
        in_specs=[VMEM] * 3 + [hbm] * 3, out_specs=VMEM,
        scratch_shapes=[pltpu.VMEM(gate.shape, BF16), pltpu.VMEM(up.shape, BF16), pltpu.VMEM(down.shape, BF16),
                        pltpu.VMEM((n - 1, rows, hidden), F32),
                        pltpu.VMEM((n, rows, hidden), BF16), pltpu.VMEM((tokens, hidden), BF16),
                        pltpu.VMEM((tokens, gate.shape[1]), BF16), pltpu.VMEM((n, tokens, cw), F32),
                        pltpu.VMEM((6, tokens // 2, cw), F32), pltpu.VMEM((2, tokens // 2, cw), F32),
                        pltpu.VMEM((n, tokens, cw), BF16), pltpu.SemaphoreType.DMA((3 * cuts,))]
        + [pltpu.SemaphoreType.DMA((6,))] * 2 + [sem] * 6,
        compiler_params=pltpu.CompilerParams(collective_id=cid, has_side_effects=True, vmem_limit_bytes=62 << 20),
        name="dense_mlp",
    )(part, res, gain, gate, up, down)


def routed_kernel(nt, nx, chunks, part_ref, res_ref, gain_ref, mask_ref, router_ref, gate_hbm, up_hbm, down_hbm, sg_hbm, su_hbm, sd_hbm, out_ref,
                  gate, up, down, sg, su, sd, tok, xt, act, comb_t, comb, sh, recv, y, po, pc, hin, ax, ay, bx, by, ox, oy, fin, wsem, shsem,
                  s1, r1, sx, rx, sy, ry, syl, ryl, sxh, rxh, sdd, rdd,
                  sp, rp, sx1, rx1, sy1, ry1, sy2, ry2, sx2, rx2, sag, rag):
    t = lax.axis_index("tp")
    ep = lax.axis_index("ep")
    x, c = ep // PAIR, lax.rem(ep, PAIR)
    o = 1 - c
    sib = {"ep": x * PAIR + o}
    rows, hidden = y.shape
    n_exp = gate.shape[0]
    experts = router_ref.shape[0]
    own = nt * rows
    side = nx * own
    total_w = tok.shape[-1]
    half = hidden // 2
    lo, hi = pl.ds(0, half), pl.ds(half, total_w - half)
    tps = range(nt - 1)
    xs = range(nx - 1)
    tp_peer = [lax.rem(t + d + 1, nt) for d in tps]
    tp_src = [lax.rem(t - d - 1 + nt, nt) for d in tps]
    x_peer = [lax.rem(x + d + 1, nx) for d in xs]
    x_src = [lax.rem(x - d - 1 + nx, nx) for d in xs]

    def to_x(p):
        return {"ep": p * PAIR + c}

    def to_t(p):
        return {"tp": p}

    def rc(src, dst, ssem, rsem, dev):
        return pltpu.make_async_remote_copy(src_ref=src, dst_ref=dst, send_sem=ssem, recv_sem=rsem, device_id=dev, device_id_type=MESH)

    sends = []

    def send(src, dst, ssem, rsem, dev):
        copy = rc(src, dst, ssem, rsem, dev)
        copy.start()
        sends.append(copy)
        return copy

    def arrived(ref, ssem, rsem, dev):
        rc(ref, ref, ssem, rsem, dev).wait_recv()

    shared_loads = [pltpu.make_async_copy(src, dst, shsem.at[k]) for k, (src, dst) in enumerate(((sg_hbm, sg), (su_hbm, su), (sd_hbm, sd)))]
    for copy in shared_loads:
        copy.start()
    weights = ((gate_hbm, gate), (up_hbm, up), (down_hbm, down))

    def load(k, e):
        return pltpu.make_async_copy(weights[k][0].at[e], weights[k][1].at[e], wsem.at[k, e])

    for e in range(n_exp):
        load(0, e).start()
        load(1, e).start()
    for e in range(n_exp):
        load(2, e).start()

    barrier = pltpu.get_barrier_semaphore()
    for p in tp_peer:
        pl.semaphore_signal(barrier, inc=1, device_id=to_t(p), device_id_type=MESH)
    for p in x_peer:
        pl.semaphore_signal(barrier, inc=1, device_id=to_x(p), device_id_type=MESH)
    pl.semaphore_signal(barrier, inc=1, device_id=sib, device_id_type=MESH)
    pl.semaphore_wait(barrier, nt + nx - 1)

    total, first = sum_tp(t, nt, rows, part_ref, recv, s1, r1)
    sends += first
    mine = (res_ref[pl.ds(t * rows, rows), :].astype(F32) + total).astype(BF16)
    y[...] = mine
    tok[c, x, t, :, pl.ds(0, hidden)] = rms_norm(mine, gain_ref[1:2, :])
    tok[c, x, t, :, pl.ds(hidden, total_w - hidden)] = mask_ref[pl.ds(t * rows, rows), :]
    row = tok.at[c, x, t]
    for d in xs:
        send(row, row, sx.at[d], rx.at[d], to_x(x_peer[d]))
    for d in tps:
        send(row, row, sy.at[d], ry.at[d], to_t(tp_peer[d]))
    send(row, row, sdd.at[0], rdd.at[0], sib)
    k = 1
    passed = []
    for d in xs:
        ref = tok.at[c, x_src[d], t]
        arrived(ref, sx.at[d], rx.at[d], to_x(x_src[d]))
        low = tok.at[c, x_src[d], t, :, lo]
        for f in tps:
            send(low, low, syl.at[d, f], ryl.at[d, f], to_t(tp_peer[f]))
        send(ref, ref, sdd.at[k], rdd.at[k], sib)
        passed.append((x_src[d], t, None))
        k += 1
    for d in tps:
        ref = tok.at[c, x, tp_src[d]]
        arrived(ref, sy.at[d], ry.at[d], to_t(tp_src[d]))
        high = tok.at[c, x, tp_src[d], :, hi]
        for f in xs:
            send(high, high, sxh.at[d, f], rxh.at[d, f], to_x(x_peer[f]))
        send(ref, ref, sdd.at[k], rdd.at[k], sib)
        passed.append((x, tp_src[d], None))
        k += 1

    for copy in shared_loads:
        copy.wait()
    a = tok[c, x, :, :, :hidden].reshape(own, hidden)
    mid = (silu(dot_nt(a, sg[...])) * dot_nt(a, su[...])).astype(BF16)
    cw = hidden // chunks
    for j in range(chunks):
        sh[:, :, j * cw:(j + 1) * cw] = dot(mid, sd[:, j * cw:(j + 1) * cw]).reshape(nt, rows, cw)

    for d in xs:
        for f in tps:
            ref = tok.at[c, x_src[d], tp_src[f], :, lo]
            arrived(ref, syl.at[d, f], ryl.at[d, f], to_t(tp_src[f]))
            send(ref, ref, sdd.at[k], rdd.at[k], sib)
            passed.append((x_src[d], tp_src[f], lo))
            k += 1
    for d in tps:
        for f in xs:
            ref = tok.at[c, x_src[f], tp_src[d], :, hi]
            arrived(ref, sxh.at[d, f], rxh.at[d, f], to_x(x_src[f]))
            send(ref, ref, sdd.at[k], rdd.at[k], sib)
            passed.append((x_src[f], tp_src[d], hi))
            k += 1
    lanes = 2 * own

    def flip(q):
        for i in range(0, nx, 2):
            at = pl.ds(pl.multiple_of(q * side + i * own, lanes), lanes)
            for j in range(0, hidden, 512):
                xt[j:j + 512, at] = tok[q, i:i + 2, :, :, j:j + 512].reshape(lanes, 512).T
            comb_t[:, at] = tok[q, i:i + 2, :, :, hidden:].reshape(lanes, total_w - hidden).astype(F32).T

    flip(c)
    ref = tok.at[o, x, t]
    arrived(ref, sdd.at[0], rdd.at[0], sib)
    for k, (i, q, cols) in enumerate(passed):
        ref = tok.at[o, i, q] if cols is None else tok.at[o, i, q, :, cols]
        arrived(ref, sdd.at[k + 1], rdd.at[k + 1], sib)
    flip(o)
    logits = dot(router_ref[...], xt[...])
    e = jnp.exp(logits - jnp.max(logits, axis=0, keepdims=True))
    comb_t[:experts, :] = e / jnp.sum(e, axis=0, keepdims=True) * comb_t[:experts, :]
    comb[...] = comb_t[pl.ds(pl.multiple_of(ep * n_exp, n_exp), n_exp), :].T

    def gate_up(e, carry):
        load(0, e).wait()
        load(1, e).wait()
        for q in range(PAIR):
            cols = xt[:, q * side:(q + 1) * side]
            act[e, q * side:(q + 1) * side, :] = (silu(dot(gate[e], cols)) * dot(up[e], cols)).astype(BF16).T
        return carry

    lax.fori_loop(0, n_exp, gate_up, 0)
    for e in range(n_exp):
        load(2, e).wait()

    hw = cw // 2
    left, right = pl.ds(0, hw), pl.ds(hw, hw)

    def expert_sum(q, j, dst, b):
        r = pl.ds(pl.multiple_of(q * side, side), side)
        w = comb[r, :]
        for e in range(n_exp):
            v = (w[:, e:e + 1] * dot(act[e, r, :], down[e, :, j * cw:(j + 1) * cw])).reshape(nx, nt, rows, cw)
            dst[b] = v if e == 0 else dst[b] + v

    pair_sends = {}
    stage1 = {}
    stage2 = {}

    def other_side(j):
        if j >= 2:
            pair_sends[j - 2].wait_send()
        expert_sum(o, j, po, j % 2)
        copy = rc(po.at[j % 2], hin.at[j], sp.at[j], rp.at[j], sib)
        copy.start()
        pair_sends[j] = copy

    def own_side(j):
        expert_sum(c, j, pc, j % 2)

    def first_sums(j):
        pair_sends[j].wait_recv()
        for i in range(nx):
            hin[j, i] = hin[j, i] + pc[j % 2, i]
        hin[j, x] = hin[j, x] + sh[:, :, j * cw:(j + 1) * cw]
        stage1[j] = [send(hin.at[j, x_peer[d], :, :, left], ax.at[j, d], sx1.at[j, d], rx1.at[j, d], to_x(x_peer[d])) for d in xs] + [
            send(hin.at[j, :, tp_peer[d], :, right], ay.at[j, d], sy1.at[j, d], ry1.at[j, d], to_t(tp_peer[d])) for d in tps]

    def second_sums(j):
        for copy in stage1[j]:
            copy.wait_recv()
        v = hin[j, x, :, :, left]
        for d in xs:
            v = v + ax[j, d]
        bx[j] = v
        v = hin[j, :, t, :, right]
        for d in tps:
            v = v + ay[j, d]
        by[j] = v
        stage2[j] = [send(bx.at[j, tp_peer[d]], ox.at[j, d], sy2.at[j, d], ry2.at[j, d], to_t(tp_peer[d])) for d in tps] + [
            send(by.at[j, x_peer[d]], oy.at[j, d], sx2.at[j, d], rx2.at[j, d], to_x(x_peer[d])) for d in xs]

    def last_sums(j):
        for copy in stage2[j]:
            copy.wait_recv()
        v = bx[j, t] + y[:, j * cw:j * cw + hw].astype(F32)
        for d in tps:
            v = v + ox[j, d]
        fin[j, t, :, left] = v.astype(BF16)
        v = by[j, x] + y[:, j * cw + hw:(j + 1) * cw].astype(F32)
        for d in xs:
            v = v + oy[j, d]
        fin[j, t, :, right] = v.astype(BF16)
        for d in tps:
            send(fin.at[j, t], fin.at[j, t], sag.at[j, d], rag.at[j, d], to_t(tp_peer[d]))

    for j in range(chunks):
        other_side(j)
        if j:
            first_sums(j - 1)
        own_side(j)
    first_sums(chunks - 1)
    second_sums(0)
    for j in range(1, chunks):
        second_sums(j)
        last_sums(j - 1)
    last_sums(chunks - 1)
    for j in range(chunks):
        for d in tps:
            arrived(fin.at[j, tp_src[d]], sag.at[j, d], rag.at[j, d], to_t(tp_src[d]))
        out_ref[:, :, j * cw:(j + 1) * cw] = fin[j]
    for j in range(max(0, chunks - 2), chunks):
        pair_sends[j].wait_send()
    for copy in sends:
        copy.wait_send()


def routed(nt, nx, cid, part, res, gain, mask, router_t, gate_t, up_t, down, sg_t, su_t, sd):
    tokens, hidden = part.shape
    rows = tokens // nt
    n_exp = gate_t.shape[0]
    total_w = hidden + mask.shape[1]
    every = PAIR * nx * tokens
    chunks = 4
    cw = hidden // chunks
    hw = cw // 2
    hbm = pl.BlockSpec(memory_space=pl.ANY)
    sem = lambda *shape: [pltpu.SemaphoreType.DMA(shape)] * 2
    f32 = lambda *shape: pltpu.VMEM(shape, F32)
    bf16 = lambda *shape: pltpu.VMEM(shape, BF16)
    mx, mt = nx - 1, nt - 1
    return pl.pallas_call(
        functools.partial(routed_kernel, nt, nx, chunks),
        out_shape=jax.ShapeDtypeStruct((nt, rows, hidden), BF16),
        in_specs=[VMEM] * 5 + [hbm] * 6, out_specs=VMEM,
        scratch_shapes=[bf16(*gate_t.shape), bf16(*up_t.shape), bf16(*down.shape), bf16(*sg_t.shape), bf16(*su_t.shape), bf16(*sd.shape),
                        bf16(PAIR, nx, nt, rows, total_w), bf16(hidden, every), bf16(n_exp, every, down.shape[1]),
                        f32(mask.shape[1], every), f32(every, n_exp), f32(nt, rows, hidden), f32(mt, rows, hidden), bf16(rows, hidden),
                        f32(2, nx, nt, rows, cw), f32(2, nx, nt, rows, cw), f32(chunks, nx, nt, rows, cw),
                        f32(chunks, mx, nt, rows, hw), f32(chunks, mt, nx, rows, hw), f32(chunks, nt, rows, hw), f32(chunks, nx, rows, hw),
                        f32(chunks, mt, rows, hw), f32(chunks, mx, rows, hw), bf16(chunks, nt, rows, cw),
                        pltpu.SemaphoreType.DMA((3, n_exp)), pltpu.SemaphoreType.DMA((3,))]
        + sem(mt) + sem(mx) + sem(mt) + sem(mx, mt) + sem(mt, mx) + sem(1 + mx + mt + 2 * mx * mt)
        + sem(chunks) + sem(chunks, mx) + sem(chunks, mt) + sem(chunks, mt) + sem(chunks, mx) + sem(chunks, mt),
        compiler_params=pltpu.CompilerParams(collective_id=cid, has_side_effects=True, vmem_limit_bytes=67_000_000),
        name="routed_layer",
    )(part, res, gain, mask, router_t, gate_t, up_t, down, sg_t, su_t, sd)


def attention_layer(layer, group, pos_ref, gain_ref, gkv_ref, wq_hbm, wkv_hbm, wuk_hbm, wuv_hbm, wo_hbm, lat_hbm, rope_hbm, lat_to, rope_to,
                    wq, wkv, wuk, wuv, wo, lat, rop, qn, q1, q2, latn, ropet, o, qsem, wsem, csem, osem):
    seqs, sh, lora = qn.shape
    heads, qk = wq.shape[:2]
    steps = sh // heads
    nope = wuk.shape[2]
    rope = qk - nope
    rh = rope // 2
    slots = lat.shape[1]
    groups = seqs // group
    q_loads = [pltpu.make_async_copy(wq_hbm.at[layer, k], wq.at[k], qsem.at[k]) for k in range(heads)]
    w_loads = [pltpu.make_async_copy(src.at[layer], dst, wsem.at[k]) for k, (src, dst) in enumerate(
        ((wuk_hbm, wuk), (wkv_hbm, wkv), (wuv_hbm, wuv), (wo_hbm, wo)))]

    def part_of(g):
        return pl.ds(g * group, group)

    def lat_load(g):
        return pltpu.make_async_copy(lat_hbm.at[layer, part_of(g)], lat.at[part_of(g)], csem.at[0, g])

    def rope_load(g):
        return pltpu.make_async_copy(rope_hbm.at[layer, part_of(g)], rop.at[part_of(g)], csem.at[1, g])

    def lat_store(g):
        return pltpu.make_async_copy(lat.at[part_of(g)], lat_to.at[layer, part_of(g)], osem.at[0, g])

    def rope_store(g):
        return pltpu.make_async_copy(rop.at[part_of(g)], rope_to.at[layer, part_of(g)], osem.at[1, g])

    def start():
        q_loads[0].start()
        w_loads[0].start()
        for copy in q_loads[1:]:
            copy.start()
        w_loads[1].start()
        for g in range(groups):
            lat_load(g).start()
            rope_load(g).start()
        w_loads[2].start()
        w_loads[3].start()

    def run(h, ct, st):
        a = rms_norm(h, gain_ref[layer:layer + 1, :])
        cos_t, sin_t = ct.T, st.T
        for k in range(heads):
            q_loads[k].wait()
            if k == 0:
                w_loads[0].wait()
            qh = dot_nt(a, wq[k, :nope, :]).astype(BF16)
            ql = dot_nt(qh, wuk[k]).astype(BF16).astype(F32)
            x1 = dot_nt(a, wq[k, nope:nope + rh, :])
            x2 = dot_nt(a, wq[k, nope + rh:, :])
            r1 = (x1 * cos_t - x2 * sin_t).astype(BF16).astype(F32)
            r2 = (x2 * cos_t + x1 * sin_t).astype(BF16).astype(F32)
            for s in range(steps):
                rows = slice(s * seqs, (s + 1) * seqs)
                qn[:, s * heads + k, :] = ql[rows]
                q1[:, s * heads + k, :] = r1[rows]
                q2[:, s * heads + k, :] = r2[rows]
        w_loads[1].wait()
        latn[...] = rms_norm(dot_nt(a, wkv[:lora, :]), gkv_ref[layer:layer + 1, :]).astype(F32)
        keys = dot_nt(wkv[lora:, :], a)
        y1, y2 = keys[:rh], keys[rh:]
        ropet[:rh, :] = (y1 * ct - y2 * st).astype(BF16)
        ropet[rh:, :] = (y2 * ct + y1 * st).astype(BF16)

        tokens = latn.shape[0]
        tok_i = lax.broadcasted_iota(jnp.int32, (tokens, slots), 0)
        slot_i = lax.broadcasted_iota(jnp.int32, (tokens, slots), 1)
        lane = lax.broadcasted_iota(jnp.int32, (rope, slots), 1)
        row16 = lax.broadcasted_iota(jnp.int32, (16, 1), 0)
        slot_q = lax.broadcasted_iota(jnp.int32, (sh, slots), 1)
        step_q = lax.broadcasted_iota(jnp.int32, (sh, slots), 0) // heads

        def attend(g, carry):
            lat_load(g).wait()
            rope_load(g).wait()
            scores = []
            for j in range(group):
                b = g * group + j
                p = pos_ref[b]
                hot = jnp.zeros((tokens, slots), jnp.bool_)
                hit = jnp.zeros((rope, slots), jnp.bool_)
                for s in range(steps):
                    new = latn[pl.ds(s * seqs + b, 1), :]
                    base = pl.multiple_of((p + s) // 16 * 16, 16)
                    blk = lat[b, pl.ds(base, 16), :].astype(F32)
                    lat[b, pl.ds(base, 16), :] = jnp.where(row16 + base == p + s, new, blk).astype(BF16)
                    hot = hot | ((tok_i == s * seqs + b) & (slot_i == p + s))
                    hit = hit | (lane == p + s)
                upd = dot(ropet[...], hot.astype(F32).astype(BF16))
                rop[b] = jnp.where(hit, upd, rop[b].astype(F32)).astype(BF16)
            for j in range(group):
                b = g * group + j
                sc = dot_nt(qn[b].astype(BF16), lat[b])
                sc = sc + dot(q1[b].astype(BF16), rop[b, :rh, :]) + dot(q2[b].astype(BF16), rop[b, rh:, :])
                sc = sc * (1.0 / math.sqrt(qk))
                scores.append(jnp.where(slot_q <= pos_ref[b] + step_q, sc, -1e30))
            for j in range(group):
                e = jnp.exp(scores[j] - jnp.max(scores[j], axis=-1, keepdims=True))
                scores[j] = (e / jnp.sum(e, axis=-1, keepdims=True)).astype(BF16)
            outs = [dot(scores[j], lat[g * group + j]).astype(BF16).astype(F32) for j in range(group)]
            for j in range(group):
                o[g * group + j] = outs[j]
            lat_store(g).start()
            rope_store(g).start()
            return carry

        lax.fori_loop(0, groups, attend, 0)
        w_loads[2].wait()
        outs = []
        for k in range(heads):
            oh = jnp.concatenate([o[:, s * heads + k, :] for s in range(steps)], axis=0).astype(BF16)
            outs.append(dot(oh, wuv[k]).astype(BF16))
        w_loads[3].wait()
        part = dot(jnp.concatenate(outs, axis=1), wo[...])
        for g in range(groups):
            lat_store(g).wait()
            rope_store(g).wait()
        return part

    return start, run


def attention_kernel(layer, group, pos_ref, h_ref, gain_ref, now_ref, freq_ref, gkv_ref, wq_hbm, wkv_hbm, wuk_hbm, wuv_hbm, wo_hbm, lat_hbm, rope_hbm, *rest):
    part_ref, lat_to, rope_to, *scratch = rest[-20:]
    start, run = attention_layer(layer, group, pos_ref, gain_ref, gkv_ref, wq_hbm, wkv_hbm, wuk_hbm, wuv_hbm, wo_hbm, lat_hbm, rope_hbm,
                                 lat_to, rope_to, *scratch)
    start()
    steps = h_ref.shape[0] // now_ref.shape[1]
    now = now_ref[...]
    angle = freq_ref[...] * jnp.concatenate([now + k for k in range(steps)], axis=1).astype(F32)
    ct, st = jnp.cos(angle), jnp.sin(angle)
    part_ref[...] = run(h_ref[...], ct, st)


def attention_scratch(tokens, seqs, group, wq_t, wkv_t, wuk, wuv, w_o, lat, rope_t):
    heads = wq_t.shape[1]
    lora, rope = lat.shape[3], rope_t.shape[2]
    sh = tokens // seqs * heads
    like = lambda w: pltpu.VMEM(w.shape[1:], BF16)
    return [like(wq_t), like(wkv_t), like(wuk), like(wuv), like(w_o), like(lat), like(rope_t),
            pltpu.VMEM((seqs, sh, lora), F32), pltpu.VMEM((seqs, sh, rope // 2), F32), pltpu.VMEM((seqs, sh, rope // 2), F32),
            pltpu.VMEM((tokens, lora), F32), pltpu.VMEM((rope, tokens), BF16), pltpu.VMEM((seqs, sh, lora), F32),
            pltpu.SemaphoreType.DMA((heads,)), pltpu.SemaphoreType.DMA((4,)),
            pltpu.SemaphoreType.DMA((2, seqs // group)), pltpu.SemaphoreType.DMA((2, seqs // group))]


def attention(layer, hidden, pos, freq, g_attn, g_kv, big, written):
    tokens, width = hidden.shape
    seqs = pos.shape[0]
    lat, rope_t = big[5:]
    group = 16
    hbm = pl.BlockSpec(memory_space=pl.ANY)
    return pl.pallas_call(
        functools.partial(attention_kernel, layer, group),
        in_specs=[pl.BlockSpec(memory_space=pltpu.SMEM)] + [VMEM] * 5 + [hbm] * (7 + len(written)),
        out_specs=[VMEM, hbm, hbm],
        input_output_aliases={13: 1, 14: 2} if written else {},
        scratch_shapes=attention_scratch(tokens, seqs, group, *big),
        out_shape=[jax.ShapeDtypeStruct((tokens, width), F32), jax.ShapeDtypeStruct(lat.shape, BF16), jax.ShapeDtypeStruct(rope_t.shape, BF16)],
        compiler_params=pltpu.CompilerParams(vmem_limit_bytes=62 << 20),
        name="attention",
    )(pos, hidden, g_attn, pos.reshape(1, -1), freq, g_kv, *big, *written)


def solution(mesh):
    tok_axes = ('dp', 'ep')
    nt = mesh.shape['tp']
    nx = mesh.shape['ep'] // PAIR

    def device_fn(emb, pos, route_ids, lat_cache, rope_cache, attn_norm, w_q, w_dkv, kv_norm, w_uk, w_uv, w_o, mlp_norm, dense_gate, dense_up, dense_down, router, shared_gate, shared_up, shared_down, expert_gate, expert_up, expert_down):
        steps, seqs, hidden = emb.shape
        own = steps * seqs
        experts = router.shape[1]
        rope = rope_cache.shape[-1]
        freq = jnp.asarray(ROPE_THETA ** (-(np.arange(rope // 2, dtype=np.float64) * 2.0 / rope)), F32).reshape(-1, 1)
        ids = route_ids.reshape(own, -1)
        lanes = -(-experts // 128) * 128
        mask = jnp.any(ids[:, :, None] == jnp.arange(lanes)[None, None, :], axis=1).astype(BF16)

        h = emb.reshape(own, hidden)
        wq_t, wkv_t = w_q.transpose(0, 2, 3, 1), w_dkv.transpose(0, 2, 1)
        uk, uv = w_uk.transpose(0, 2, 1, 3), w_uv.transpose(0, 2, 1, 3)
        rope_t = rope_cache.transpose(0, 1, 3, 2)
        big = (wq_t, wkv_t, uk, uv, w_o, lat_cache, rope_t)
        part, lat, rop = attention(0, h, pos, freq, attn_norm, kv_norm, big, ())
        h = dense_mlp(nt, 0, part, h, mlp_norm, dense_gate, dense_up, dense_down)
        part, lat, rop = attention(1, h, pos, freq, attn_norm, kv_norm, big, (lat, rop))
        out = routed(nt, nx, 1, part, h, mlp_norm, mask, router.T, expert_gate.transpose(0, 2, 1), expert_up.transpose(0, 2, 1), expert_down, shared_gate.T, shared_up.T, shared_down)
        return out.reshape(steps, seqs, hidden), lat, rop.transpose(0, 1, 3, 2)

    in_specs = (P(None, tok_axes, None), P(tok_axes), P(None, tok_axes, None), P(None, tok_axes, None, None), P(None, tok_axes, None, None), P(), P(None, None, 'tp', None), P(), P(), P(None, None, 'tp', None), P(None, None, 'tp', None), P(None, 'tp', None), P(), P(None, 'tp'), P(None, 'tp'), P('tp', None), P(), P(None, 'tp'), P(None, 'tp'), P('tp', None), P('ep', None, 'tp'), P('ep', None, 'tp'), P('ep', 'tp', None))
    out_specs = (P(None, tok_axes, None), P(None, tok_axes, None, None), P(None, tok_axes, None, None))
    return jax.shard_map(device_fn, mesh=mesh, in_specs=in_specs, out_specs=out_specs, check_vma=False)
```
